256 devices in a mesh: section: 4 (over y), expert: 64 (over x, z, core).
Axes of the slice: x: 4, y: 4, z: 8, core: 2. Of those that a mesh axis runs over, the one named last changes fastest.
Arguments:
- reference_act: bfloat16 [4, 4096, 2048], P('section', 'expert'), may hold values from -6 to 6
- codes: int32 [4, 4096, 2048], P('section', 'expert'), may hold values from -127 to 127
- scale_index: int32 [4, 4096], P('section', 'expert'), may hold values from 0 to 15
- scale_table: float32 [16], replicated, may hold values from 0.002 to 0.02
- norm_gain: float32 [4, 2048], P('section'), may hold values from 0.25 to 1.75
- routes_fwd: int32 [4, 4096, 8], P('section', 'expert'), may hold values from 0 to 63, all different within a row; in each aligned block of 64 rows (0 to 63, 64 to 127, ..., all dimensions but the last counted through in order) at most 12 rows name the same one
- probs_fwd: float32 [4, 4096, 8], P('section', 'expert'), may hold values from 0.03 to 0.4
- gate_weight: bfloat16 [4, 64, 2048, 768], P('section', 'expert'), may hold values from -0.125 to 0.125
- up_weight: bfloat16 [4, 64, 2048, 768], P('section', 'expert'), may hold values from -0.125 to 0.125
- down_weight: bfloat16 [4, 64, 768, 2048], P('section', 'expert'), may hold values from -0.21875 to 0.21875
- saved_input: bfloat16 [4, 4096, 2048], P('section', 'expert'), may hold values from -6 to 6
- routes_bwd: int32 [4, 4096, 8], P('section', 'expert'), may hold values from 0 to 63, all different within a row; in each aligned block of 64 rows (0 to 63, 64 to 127, ..., all dimensions but the last counted through in order) at most 12 rows name the same one
- probs_bwd: float32 [4, 4096, 8], P('section', 'expert'), may hold values from 0.03 to 0.4
- saved_preact: bfloat16 [4, 64, 768, 1536], P('section', 'expert'), may hold values from -8 to 8
- cotangent: bfloat16 [4, 4096, 2048], P('section', 'expert'), may hold values from -6 to 6
Outputs:
- mixed: bfloat16 [4, 4096, 2048], P('section', 'expert')
- grad_input: bfloat16 [4, 4096, 2048], P('section', 'expert')
The draws below stay inside these ranges and needn't reach their ends.
Inputs may be any that keep to these rules, and one draw needn't show every extreme that they name: `routes_fwd`: the 8 ids of a token differ; among the tokens of one device no expert is named more than 12 times, a bound that some block reaches. `routes_bwd`: the 8 ids of a token differ; among the tokens of one device no expert is named more than 12 times, a bound that some block reaches.
All inputs are finite; a program needn't handle non-finite values.
Results may differ from the reference program's by a relative error of at most 0.0051.
Values may be sent and summed in bfloat16 or wider, within the bound.
A program may use at most 128 MiB of HBM per device.

```python
import math
import jax
import jax.numpy as jnp
import numpy as np
from jax import lax

D = 2048
FF = 768
TOP = 8
TOK_DEV = 64
LEVELS = 16
SECTIONS = 4
EXPERTS = 64
TOKENS = 4096
CAP = 12


def touch_ends(array, own_key, least, top_value):
    shape = array.shape
    index_at = [jax.random.randint(jax.random.fold_in(own_key, axis), (), 0, shape[axis]) for axis in range(len(shape))]
    array = array.at[tuple(index_at)].set(least)
    longest = shape.index(max(shape))
    index_at[longest] = (index_at[longest] + 1) % shape[longest]
    return array.at[tuple(index_at)].set(top_value)


def steps_of(own_key, shape, shards, least, largest):
    def one(axis_at, blocks):
        steps = jax.random.uniform(jax.random.fold_in(jax.random.fold_in(own_key, 6), axis_at), (blocks,), jnp.float32, least / len(shards), largest / len(shards))
        return jnp.repeat(jnp.exp(steps), shape[axis_at] // blocks).reshape((-1,) + (1,) * (len(shape) - axis_at - 1))

    level = one(*shards[0])
    for cut in shards[1:]:
        level = level * one(*cut)
    return level


def routed_block(key, own, number, rows, count, top, limit, skew):
    ranking = jax.random.permutation(key, count)
    crowded, common = shares(count, rows * top, limit, skew, True), shares(count, rows * top, limit, skew, False)
    places = jnp.arange(count)

    def named(sizes, offset_by):
        used = int((sizes > 0).sum())
        fixed = max(1, used // 4)
        passed = fixed + (places - fixed + offset_by * (used - fixed)) % max(1, count - fixed)
        return jnp.zeros((count,), jnp.int32).at[ranking[jnp.where(places < fixed, places, passed)]].set(jnp.asarray(sizes, jnp.int32))

    sizes = jnp.where(number % 4 == 0, named(crowded, number // 4), named(common, number - number // 4 - 1))
    mixed = jax.random.permutation(jax.random.fold_in(own, 3), count)
    donor, taker = mixed[0:count // 2 * 2:2], mixed[1:count // 2 * 2:2]
    margin = jnp.minimum(sizes[donor] - 1, limit - sizes[taker]) // 2
    margin = jnp.where((donor == ranking[0]) | (taker == ranking[0]) | (sizes[taker] == 0), 0, jnp.maximum(margin, 0))
    passed = jax.random.randint(jax.random.fold_in(own, 4), (count // 2,), 0, 1 << 20) % (margin + 1)
    sizes = sizes.at[donor].add(-passed).at[taker].add(passed)
    items = jnp.searchsorted(jnp.cumsum(sizes), jnp.arange(rows * top), side="right").astype(jnp.int32)
    grid = items.reshape(top, rows).T
    grid = grid[jax.random.permutation(jax.random.fold_in(own, 1), rows)]
    offset_by = jax.random.randint(jax.random.fold_in(own, 2), (rows, 1), 0, top)
    return jnp.take_along_axis(grid, (jnp.arange(top)[None, :] + offset_by) % top, axis=1)


def shares(number_of, total, reach, lean, full):
    weights = [(1 << 20) // math.isqrt(rank ** lean) + 1 for rank in range(1, number_of + 1)]
    largest = reach if full else min(reach, max(-(-total // number_of), total * weights[0] // sum(weights)))
    least = 1 if total - largest >= number_of - 1 else 0
    counts, spare = [largest] + [least] * (number_of - 1), total - largest - least * (number_of - 1)
    while spare > 0:
        movable = [i for i in range(1, number_of) if counts[i] < largest] or [i for i in range(1, number_of) if counts[i] < reach]
        mass, budget = sum([weights[i] for i in movable]), spare
        for i in movable:
            addition = min(reach - counts[i], max(1, budget * weights[i] // mass), spare)
            counts[i] = counts[i] + addition
            spare = spare - addition
    return np.array(counts)


def normal_values(key, shape, width, most, cuts=(), kind=jnp.bfloat16):
    values = width * jax.random.normal(key, shape, jnp.float32)
    if cuts:
        values = values * steps_of(key, shape, cuts, -0.22, 0.18)
    return jnp.clip(values, -most, most).astype(kind)


def setup_inputs(seed: int = 0) -> dict:
    key_of = jax.random.split(jax.random.key(seed), 16)
    reference_act = normal_values(key_of[0], (SECTIONS, TOKENS, D), 1.0, 6.0, ((0, 4), (1, 64)))
    codes = touch_ends(jax.random.randint(key_of[1], (SECTIONS, TOKENS, D), -127, 128), jax.random.fold_in(key_of[1], 1), -127, 127).astype(jnp.int32)
    scale_index = touch_ends(jax.random.randint(key_of[2], (SECTIONS, TOKENS), 0, LEVELS), jax.random.fold_in(key_of[2], 1), 0, LEVELS - 1).astype(jnp.int32)
    scale_table = jnp.clip(jnp.exp(jax.random.uniform(key_of[3], (LEVELS,), jnp.float32, math.log(0.002), math.log(0.02))), 0.002, 0.02)
    norm_gain = jnp.clip(1.0 + 0.15 * jax.random.normal(key_of[4], (SECTIONS, D), jnp.float32), 0.25, 1.75)
    routes_fwd_keys = jax.random.split(jax.random.fold_in(key_of[5], 1), SECTIONS * TOKENS // TOK_DEV)
    routes_fwd_turns = jax.random.permutation(jax.random.fold_in(key_of[5], 3), SECTIONS * TOKENS // TOK_DEV)
    routes_fwd = jax.vmap(lambda own, number: routed_block(jax.random.fold_in(key_of[5], 2), own, number, TOK_DEV, EXPERTS, TOP, CAP, 2))(routes_fwd_keys, routes_fwd_turns).reshape((SECTIONS, TOKENS, TOP))
    probs_fwd = jnp.clip(jnp.exp(math.log(0.4) - 2.5902672 * jax.random.uniform(key_of[6], (SECTIONS, TOKENS, TOP), jnp.float32) ** steps_of(key_of[6], (SECTIONS, TOKENS, TOP), ((0, 4), (1, 64)), -0.2, 0.2)), 0.03, 0.4)
    gate_weight = normal_values(key_of[7], (SECTIONS, EXPERTS, D, FF), D ** -0.5, 0.125, ((0, 4), (1, 64)))
    up_weight = normal_values(key_of[8], (SECTIONS, EXPERTS, D, FF), D ** -0.5, 0.125, ((0, 4), (1, 64)))
    down_weight = normal_values(key_of[9], (SECTIONS, EXPERTS, FF, D), FF ** -0.5, 0.21875, ((0, 4), (1, 64)))
    saved_input = normal_values(key_of[10], (SECTIONS, TOKENS, D), 1.0, 6.0, ((0, 4), (1, 64)))
    routes_bwd_keys = jax.random.split(jax.random.fold_in(key_of[11], 1), SECTIONS * TOKENS // TOK_DEV)
    routes_bwd_turns = jax.random.permutation(jax.random.fold_in(key_of[11], 3), SECTIONS * TOKENS // TOK_DEV)
    routes_bwd = jax.vmap(lambda own, number: routed_block(jax.random.fold_in(key_of[11], 2), own, number, TOK_DEV, EXPERTS, TOP, CAP, 2))(routes_bwd_keys, routes_bwd_turns).reshape((SECTIONS, TOKENS, TOP))
    probs_bwd = jnp.clip(jnp.exp(math.log(0.4) - 2.5902672 * jax.random.uniform(key_of[12], (SECTIONS, TOKENS, TOP), jnp.float32) ** steps_of(key_of[12], (SECTIONS, TOKENS, TOP), ((0, 4), (1, 64)), -0.2, 0.2)), 0.03, 0.4)
    saved_preact = normal_values(key_of[13], (SECTIONS, EXPERTS, EXPERTS * CAP, 2 * FF), 1.5, 8.0, ((0, 4), (1, 64)))
    cotangent = normal_values(key_of[14], (SECTIONS, TOKENS, D), 1.0, 6.0, ((0, 4), (1, 64)))
    return {"reference_act": reference_act, "codes": codes, "scale_index": scale_index, "scale_table": scale_table, "norm_gain": norm_gain, "routes_fwd": routes_fwd, "probs_fwd": probs_fwd, "gate_weight": gate_weight, "up_weight": up_weight, "down_weight": down_weight, "saved_input": saved_input, "routes_bwd": routes_bwd, "probs_bwd": probs_bwd, "saved_preact": saved_preact, "cotangent": cotangent}


EPSILON = 1e-06

def inverse_rms(values):
    return lax.rsqrt(lax.optimization_barrier(jnp.mean(values * values, axis=-1, keepdims=True)) + EPSILON)

def slot_targets(routes, experts, capacity):
    flat_ids = routes.reshape(-1).astype(jnp.int32)
    onehot = (flat_ids[:, None] == jnp.arange(experts, dtype=jnp.int32)[None, :]).astype(jnp.int32)
    earlier = jnp.cumsum(onehot, axis=0) - onehot
    slot_index = lax.optimization_barrier(jnp.sum(earlier * onehot, axis=1))
    return (flat_ids * capacity + slot_index).astype(jnp.int32)

def dispatch(rows, targets, experts, capacity):
    copies_each = targets.shape[0] // rows.shape[0]
    copies = jnp.repeat(rows, copies_each, axis=0)
    buffer = jnp.zeros((experts * capacity, rows.shape[1]), rows.dtype)
    return buffer.at[targets].set(copies)

def collect(buffer, targets, weights):
    picked = buffer[targets].astype(jnp.float32).reshape(weights.shape[0], weights.shape[1], buffer.shape[1])
    return lax.optimization_barrier(jnp.sum(picked * weights[:, :, None], axis=1))

def expert_forward(rows, gate_matrix, up_matrix, down_matrix):
    gate_act = jnp.dot(rows, gate_matrix, preferred_element_type=jnp.float32)
    up_act = jnp.dot(rows, up_matrix, preferred_element_type=jnp.float32)
    hidden = (gate_act * jax.nn.sigmoid(gate_act) * up_act).astype(jnp.bfloat16)
    return jnp.dot(hidden, down_matrix, preferred_element_type=jnp.float32).astype(jnp.bfloat16)

def expert_backward(grad_rows, stored, gate_matrix, up_matrix, down_matrix):
    hidden_units = gate_matrix.shape[1]
    gate_act = stored[:, :hidden_units].astype(jnp.float32)
    up_act = stored[:, hidden_units:].astype(jnp.float32)
    contract = (((1,), (1,)), ((), ()))
    grad_hidden = lax.dot_general(grad_rows, down_matrix, contract, preferred_element_type=jnp.float32)
    sigma = jax.nn.sigmoid(gate_act)
    silu_value = gate_act * sigma
    slope = sigma * (1.0 + gate_act * (1.0 - sigma))
    grad_gate = (grad_hidden * up_act * slope).astype(jnp.bfloat16)
    grad_up = (grad_hidden * silu_value).astype(jnp.bfloat16)
    result = lax.dot_general(grad_gate, gate_matrix, contract, preferred_element_type=jnp.float32)
    result = result + lax.dot_general(grad_up, up_matrix, contract, preferred_element_type=jnp.float32)
    return result.astype(jnp.bfloat16)

def through_experts(rows, routes, weights, expert_fn, expert_args):
    model_width = rows.shape[1]
    blocks = rows.reshape(EXPERTS, TOK_DEV, model_width)
    targets = jax.vmap(lambda block_routes: slot_targets(block_routes, EXPERTS, CAP))(routes.reshape(EXPERTS, TOK_DEV, TOP))
    sent = jax.vmap(lambda block_rows, block_targets: dispatch(block_rows, block_targets, EXPERTS, CAP))(blocks, targets)
    arrived = sent.reshape(EXPERTS, EXPERTS, CAP, model_width).transpose(1, 0, 2, 3).reshape(EXPERTS, EXPERTS * CAP, model_width)
    produced = lax.map(lambda member: expert_fn(*member), (arrived,) + expert_args)
    returned = produced.reshape(EXPERTS, EXPERTS, CAP, model_width).transpose(1, 0, 2, 3).reshape(EXPERTS, EXPERTS * CAP, model_width)
    combined = jax.vmap(collect)(returned, targets, weights.reshape(EXPERTS, TOK_DEV, TOP))
    return combined.reshape(EXPERTS * TOK_DEV, model_width)

def reference(reference_act, codes, scale_index, scale_table, norm_gain, routes_fwd, probs_fwd, gate_weight, up_weight, down_weight, saved_input, routes_bwd, probs_bwd, saved_preact, cotangent):
    row_scale = scale_table[scale_index]
    delta_rows = (codes.astype(jnp.float32) * row_scale[:, :, None]).astype(jnp.bfloat16)
    received = jnp.concatenate([jnp.zeros_like(delta_rows[:1]), delta_rows[:-1]], axis=0)
    grad_out = jnp.roll(cotangent, -1, axis=0)
    outputs = []
    gradients = []
    for section_index in range(SECTIONS):
        inputs_now = reference_act[section_index].astype(jnp.float32) + received[section_index].astype(jnp.float32)
        gain_row = norm_gain[section_index]
        normed = (inputs_now * inverse_rms(inputs_now) * gain_row).astype(jnp.bfloat16)
        forward_args = (gate_weight[section_index], up_weight[section_index], down_weight[section_index])
        mixed = inputs_now + through_experts(normed, routes_fwd[section_index], probs_fwd[section_index], expert_forward, forward_args)
        outputs.append(mixed.astype(jnp.bfloat16))
        backward_args = (saved_preact[section_index], gate_weight[section_index], up_weight[section_index], down_weight[section_index])
        grad_normed = through_experts(grad_out[section_index], routes_bwd[section_index], probs_bwd[section_index], expert_backward, backward_args)
        saved_now = saved_input[section_index].astype(jnp.float32)
        scale_now = inverse_rms(saved_now)
        weighted = grad_normed * gain_row
        projection = lax.optimization_barrier(jnp.mean(weighted * saved_now, axis=-1, keepdims=True))
        grad_now = grad_out[section_index].astype(jnp.float32) + scale_now * weighted - saved_now * scale_now * scale_now * scale_now * projection
        gradients.append(grad_now.astype(jnp.bfloat16))
    return (jnp.stack(outputs), jnp.stack(gradients))
```

```python
import functools

import jax
import jax.numpy as jnp
from jax import lax
from jax.experimental import pallas as pl
from jax.experimental.pallas import tpu as pltpu
from jax.sharding import PartitionSpec as P

EPSILON = 1e-06
NX, NZ = 4, 8
ROWS = 64
CAP = 12
GROUP = 4
SLOTS = GROUP * CAP
TOKENS = GROUP * ROWS
CHUNK = 4 * SLOTS
COLS = 512
MESH = pl.DeviceIdType.MESH
F32, BF16 = jnp.float32, jnp.bfloat16


def kernel(
    ref_h, codes_h, scale_h, gain_h, meta_h, saved_h, cot_h, gate_h, up_h, down_h, pre_h,
    mixed_o, grad_o,
    ref_v, codes_v, scale_v, gain_v, saved_v, gate_v, up_v, down_v, pre_v,
    dsend_v, drecv_v, gout_v, norm_v, inputs_v, meta_v, tgt_v, wgt_v,
    ag, send, arr, ret, d2, rs,
    ld_s, y_s, y_r, m_s, m_r, ring_s, ring_r, sib_s, sib_r, x_s, x_r, t_s, t_r, d_s, d_r, r_s, r_r,
):
    s, x, z, c = (lax.axis_index(a) for a in ("section", "x", "z", "core"))
    width = ref_v.shape[1]
    ffn = gate_v.shape[1]
    own = z * 2 + c

    def at_z(off):
        return lax.rem(z + (off + NZ), NZ)

    def at_x(off):
        return lax.rem(x + off, NX)

    def rows_of(zz):
        return pl.ds(pl.multiple_of((zz * 2 + c) * ROWS, ROWS), ROWS)

    def rcopy(src, dst, ssem, rsem, dev):
        return pltpu.make_async_remote_copy(
            src_ref=src, dst_ref=dst, send_sem=ssem, recv_sem=rsem,
            device_id=dev, device_id_type=MESH,
        )

    def arrived(dst, ssem, rsem):
        rcopy(dst, dst, ssem, rsem, {"core": 1 - c}).wait_recv()

    loads = [
        (meta_h, meta_v.at[own]), (codes_h, codes_v), (scale_h, scale_v), (ref_h, ref_v), (gain_h, gain_v),
        (saved_h, saved_v), (down_h, down_v), (gate_h, gate_v), (up_h, up_v), (pre_h, pre_v),
    ]
    loads = [pltpu.make_async_copy(a, b, ld_s.at[k]) for k, (a, b) in enumerate(loads)]
    for ld in loads:
        ld.start()

    peers = [{"section": lax.rem(s + 1, 4)}, {"section": lax.rem(s + 3, 4)}]
    peers += [{"x": at_x(d)} for d in (1, 2, 3)]
    column = [(dz, dc) for dz in range(NZ) for dc in (0, 1) if (dz, dc) != (0, 0)]
    peers += [{"z": at_z(dz), "core": lax.rem(c + dc, 2)} for dz, dc in column]
    barrier = pltpu.get_barrier_semaphore()
    for dev in peers:
        pl.semaphore_signal(barrier, inc=1, device_id=dev, device_id_type=MESH)
    pl.semaphore_wait(barrier, len(peers))

    y_cot = rcopy(cot_h, gout_v, y_s.at[0], y_r.at[0], peers[1])
    y_cot.start()
    loads[0].wait()
    metas = []
    for k, (dz, dc) in enumerate(column):
        cp = rcopy(meta_v.at[own], meta_v.at[own], m_s.at[k], m_r.at[k], peers[5 + k])
        cp.start()
        metas.append(cp)
    loads[1].wait()
    loads[2].wait()
    dsend_v[...] = (codes_v[...].astype(F32) * scale_v[...]).astype(BF16)
    y_delta = rcopy(dsend_v, drecv_v, y_s.at[1], y_r.at[1], peers[0])
    y_delta.start()
    for k, (dz, dc) in enumerate(column):
        src = lax.rem(z - dz + NZ, NZ) * 2 + lax.rem(c + dc, 2)
        arrived(meta_v.at[src], m_s.at[k], m_r.at[k])

    both = meta_v[...].reshape(16 * 16, 128)
    turned = pltpu.roll(both, ROWS, 1).reshape(NZ, 2, 16, 128)
    both = both.reshape(NZ, 2, 16, 128)
    low = lax.broadcasted_iota(jnp.int32, (NZ, 8, 128), 2) < ROWS
    tri_r = lax.broadcasted_iota(jnp.int32, (128, 128), 0)
    tri_c = lax.broadcasted_iota(jnp.int32, (128, 128), 1)
    tri = jnp.where((tri_r < tri_c) & ((tri_r < ROWS) == (tri_c < ROWS)), 1.0, 0.0).astype(BF16)
    lane = lax.broadcasted_iota(jnp.int32, (NX * NZ, 128), 1)
    zrow = lax.broadcasted_iota(jnp.int32, (NX * NZ, 128), 0)
    shift = jnp.where(lane < ROWS, 0, CAP) + lax.rem(zrow, 2) * (2 * CAP)
    for p in (0, 1):
        if p == 0:
            routes = jnp.where(low, both[:, 0, :8], turned[:, 1, :8])
            probs = jnp.where(low, both[:, 0, 8:], turned[:, 1, 8:])
        else:
            routes = jnp.where(low, turned[:, 0, :8], both[:, 1, :8])
            probs = jnp.where(low, turned[:, 0, 8:], both[:, 1, 8:])
        named, weights = [], []
        for xe in range(NX):
            expert = (xe * 16 + own).astype(F32)
            hit = routes == expert
            named.append(jnp.sum(jnp.where(hit, 1.0, 0.0), axis=1))
            weights.append(jnp.sum(jnp.where(hit, probs, 0.0), axis=1))
        named = jnp.concatenate(named, axis=0)
        earlier = jnp.dot(named.astype(BF16), tri, preferred_element_type=F32)
        tgt_v[p] = jnp.where(named > 0.5, earlier + shift.astype(F32), -1.0)
        wgt_v[p] = jnp.concatenate(weights, axis=0)

    slot_iota = lax.broadcasted_iota(jnp.int32, (SLOTS, TOKENS), 0).astype(F32)

    def row_pair(ref, p, xe, g):
        at = xe * NZ + 2 * g
        return jnp.concatenate([ref[p, pl.ds(at, 1), :], ref[p, pl.ds(at + 1, 1), :]], axis=1)

    x_copies = []

    def dispatch(p, n, g):
        pick = jnp.concatenate(
            [jnp.where(slot_iota == row_pair(tgt_v, p, at_x(d), g), 1.0, 0.0) for d in range(NX)], axis=0
        ).astype(BF16)
        here = pl.ds(pl.multiple_of(x * CHUNK + g * SLOTS, 16), SLOTS)
        for k in range(0, width, COLS):
            cols = pl.ds(k, COLS)
            block = ag[p, pl.ds(pl.multiple_of(g * TOKENS, TOKENS), TOKENS), cols]
            rows = jnp.dot(pick, block, preferred_element_type=F32).astype(BF16)
            arr[p, here, cols] = rows[:SLOTS]
            send[p, pl.ds(n * 3 * SLOTS, 3 * SLOTS), cols] = rows[SLOTS:]
        for d in (1, 2, 3):
            cp = rcopy(
                send.at[p, pl.ds((n * 3 + d - 1) * SLOTS, SLOTS)], arr.at[p, here],
                x_s.at[p, n * 3 + d - 1], x_r.at[p, n * 3 + d - 1], {"x": at_x(d)},
            )
            cp.start()
            x_copies.append(cp)

    ring_copies = []

    def hop(p, k, src):
        zz = at_z(1 - k) if k > 0 else at_z(-1 - k)
        q = k - 1 if k > 0 else 3 - k
        cp = rcopy(src, ag.at[p, rows_of(zz)], ring_s.at[p, q], ring_r.at[p, q], {"z": at_z(1 if k > 0 else -1)})
        cp.start()
        ring_copies.append(cp)

    def to_sibling(p, q, zz, src):
        cp = rcopy(src, ag.at[p, rows_of(zz)], sib_s.at[p, q], sib_r.at[p, q], {"core": 1 - c})
        cp.start()
        ring_copies.append(cp)

    def ring_wait(p, k):
        zz = at_z(-k)
        q = k - 1 if k > 0 else 3 - k
        arrived(ag.at[p, rows_of(zz)], ring_s.at[p, q], ring_r.at[p, q])
        return zz

    def sib_wait(p, q, zz):
        there = pl.ds(pl.multiple_of((zz * 2 + 1 - c) * ROWS, ROWS), ROWS)
        arrived(ag.at[p, there], sib_s.at[p, q], sib_r.at[p, q])

    half = z // 2
    odd = 2 * lax.rem(z, 2) - 1
    order = [half, lax.rem(half + odd + 4, 4), lax.rem(half - odd + 4, 4), lax.rem(half + 2, 4)]

    def start_ring(p, src):
        hop(p, 1, src)
        hop(p, -1, src)
        to_sibling(p, 0, z, src)
        ag[p, rows_of(z), :] = src[...]

    def step(p, k):
        zz = ring_wait(p, k)
        if k < 4:
            hop(p, k + 1, ag.at[p, rows_of(zz)])
        to_sibling(p, k, zz, ag.at[p, rows_of(zz)])
        if k < 4:
            zm = ring_wait(p, -k)
            if k < 3:
                hop(p, -k - 1, ag.at[p, rows_of(zm)])
            to_sibling(p, 4 + k, zm, ag.at[p, rows_of(zm)])

    def settle(p, k):
        sib_wait(p, k, at_z(-k))
        if 0 < k < 4:
            sib_wait(p, 4 + k, at_z(k))

    y_cot.wait_recv()
    start_ring(0, gout_v)

    y_delta.wait_recv()
    loads[3].wait()
    loads[4].wait()
    first = jnp.where(s > 0, 1.0, 0.0)
    inputs = ref_v[...].astype(F32) + drecv_v[...].astype(F32) * first
    inputs_v[...] = inputs
    inverse = lax.rsqrt(jnp.mean(inputs * inputs, axis=-1, keepdims=True) + EPSILON)
    norm_v[...] = (inputs * inverse * gain_v[...]).astype(BF16)

    step(0, 1)
    settle(0, 0)
    settle(0, 1)
    dispatch(0, 0, order[0])
    step(0, 2)
    settle(0, 2)
    dispatch(0, 1, order[1])
    step(0, 3)
    start_ring(1, norm_v)
    settle(0, 3)
    dispatch(0, 2, order[2])
    step(0, 4)
    settle(0, 4)
    dispatch(0, 3, order[3])
    step(1, 1)
    settle(1, 0)
    settle(1, 1)
    dispatch(1, 0, order[0])
    step(1, 2)
    settle(1, 2)
    dispatch(1, 1, order[1])
    step(1, 3)
    settle(1, 3)
    dispatch(1, 2, order[2])
    step(1, 4)
    settle(1, 4)
    dispatch(1, 3, order[3])

    def slots_arrived(p):
        for n in range(4):
            for d in (1, 2, 3):
                where = pl.ds(pl.multiple_of(lax.rem(x - d + NX, NX) * CHUNK + order[n] * SLOTS, 16), SLOTS)
                arrived(arr.at[p, where], x_s.at[p, n * 3 + d - 1], x_r.at[p, n * 3 + d - 1])

    across = (((1,), (1,)), ((), ()))

    slots_arrived(0)
    for ld in loads[5:]:
        ld.wait()

    @pl.loop(0, NX)
    def _(k):
        at = pl.ds(pl.multiple_of(k * CHUNK, CHUNK), CHUNK)
        hidden = lax.dot_general(arr[0, at, :], down_v[...], across, preferred_element_type=F32)
        gate_act = pre_v[at, :ffn].astype(F32)
        up_act = pre_v[at, ffn:].astype(F32)
        sigma = jax.nn.sigmoid(gate_act)
        grad_gate = (hidden * up_act * sigma * (1.0 + gate_act * (1.0 - sigma))).astype(BF16)
        grad_up = (hidden * gate_act * sigma).astype(BF16)
        for j in range(0, width, COLS):
            total = lax.dot_general(grad_gate, gate_v[j : j + COLS, :], across, preferred_element_type=F32)
            total += lax.dot_general(grad_up, up_v[j : j + COLS, :], across, preferred_element_type=F32)
            arr[0, at, j : j + COLS] = total.astype(BF16)

    t_copies = []

    def give_back(p):
        for n in (0, 1, 2, 3):
            g = order[3 - n]
            for d in (1, 2, 3):
                where = pl.ds(pl.multiple_of(at_x(d) * CHUNK + g * SLOTS, 16), SLOTS)
                land = pl.ds(pl.multiple_of(n * CHUNK + x * SLOTS, 16), SLOTS)
                cp = rcopy(
                    arr.at[p, where], ret.at[p, land],
                    t_s.at[p, n * 3 + d - 1], t_r.at[p, n * 3 + d - 1], {"x": at_x(d)},
                )
                cp.start()
                t_copies.append(cp)

    give_back(0)

    slots_arrived(1)

    @pl.loop(0, NX)
    def _(k):
        at = pl.ds(pl.multiple_of(k * CHUNK, CHUNK), CHUNK)
        rows = arr[1, at, :]
        gate_act = jnp.dot(rows, gate_v[...], preferred_element_type=F32)
        up_act = jnp.dot(rows, up_v[...], preferred_element_type=F32)
        hidden = (gate_act * jax.nn.sigmoid(gate_act) * up_act).astype(BF16)
        for j in range(0, width, COLS):
            total = jnp.dot(hidden, down_v[:, j : j + COLS], preferred_element_type=F32)
            arr[1, at, j : j + COLS] = total.astype(BF16)

    give_back(1)

    for cp in ring_copies:
        cp.wait_send()

    d_copies, r_copies = [], []

    def combine(p, n):
        g = order[3 - n]
        for d in (1, 2, 3):
            land = pl.ds(pl.multiple_of(n * CHUNK + lax.rem(x - d + NX, NX) * SLOTS, 16), SLOTS)
            arrived(ret.at[p, land], t_s.at[p, n * 3 + d - 1], t_r.at[p, n * 3 + d - 1])
        mine = pl.ds(pl.multiple_of(n * CHUNK + x * SLOTS, 16), SLOTS)
        here = pl.ds(pl.multiple_of(x * CHUNK + g * SLOTS, 16), SLOTS)
        ret[p, mine, :] = arr[p, here, :]
        share = jnp.concatenate(
            [
                jnp.where(slot_iota == row_pair(tgt_v, p, xe, g), row_pair(wgt_v, p, xe, g), 0.0)
                for xe in range(NX)
            ],
            axis=0,
        )
        share = share.T.astype(BF16)
        tokens = pl.ds(pl.multiple_of(g * TOKENS, TOKENS), TOKENS)
        for k in range(0, width, COLS):
            cols = pl.ds(k, COLS)
            got = jnp.dot(share, ret[p, pl.ds(n * CHUNK, CHUNK), cols], preferred_element_type=F32)
            ag[p, tokens, cols] = got.astype(BF16)
        for h in (0, 1):
            away = pl.ds(pl.multiple_of(g * TOKENS + h * 128 + (1 - c) * ROWS, ROWS), ROWS)
            cp = rcopy(
                ag.at[p, away], d2.at[p, pl.ds((n * 2 + h) * ROWS, ROWS)],
                d_s.at[p, n * 2 + h], d_r.at[p, n * 2 + h], {"core": 1 - c},
            )
            cp.start()
            d_copies.append(cp)
        for h in (0, 1):
            land = pl.ds((n * 2 + h) * ROWS, ROWS)
            arrived(d2.at[p, land], d_s.at[p, n * 2 + h], d_r.at[p, n * 2 + h])
            stay = pl.ds(pl.multiple_of(g * TOKENS + h * 128 + c * ROWS, ROWS), ROWS)
            ag[p, stay, :] = (ag[p, stay, :].astype(F32) + d2[p, land, :].astype(F32)).astype(BF16)

    def pass_on(p, k):
        zz = at_z(5 - k) if k > 0 else at_z(-4 - k)
        q = k - 1 if k > 0 else 3 - k
        there = rows_of(zz)
        if k not in (1, -1):
            arrived(rs.at[p, q - 1], r_s.at[p, q - 1], r_r.at[p, q - 1])
            ag[p, there, :] = (ag[p, there, :].astype(F32) + rs[p, q - 1].astype(F32)).astype(BF16)
        cp = rcopy(ag.at[p, there], rs.at[p, q], r_s.at[p, q], r_r.at[p, q], {"z": at_z(1 if k > 0 else -1)})
        cp.start()
        r_copies.append(cp)

    def owned(p):
        for q in (3, 6):
            arrived(rs.at[p, q], r_s.at[p, q], r_r.at[p, q])
        return ag[p, rows_of(z), :].astype(F32) + rs[p, 3].astype(F32) + rs[p, 6].astype(F32)

    def reduce_ring(p):
        combine(p, 0)
        pass_on(p, 1)
        combine(p, 1)
        pass_on(p, -1)
        pass_on(p, 2)
        combine(p, 2)
        pass_on(p, -2)
        pass_on(p, 3)
        combine(p, 3)
        pass_on(p, -3)
        pass_on(p, 4)

    reduce_ring(0)
    weighted = owned(0) * gain_v[...]
    saved = saved_v[...].astype(F32)
    scale = lax.rsqrt(jnp.mean(saved * saved, axis=-1, keepdims=True) + EPSILON)
    projection = jnp.mean(weighted * saved, axis=-1, keepdims=True)
    grad_o[...] = (
        gout_v[...].astype(F32) + scale * weighted - saved * (scale * scale * scale * projection)
    ).astype(BF16)

    reduce_ring(1)
    mixed_o[...] = (inputs_v[...] + owned(1)).astype(BF16)

    y_cot.wait_send()
    y_delta.wait_send()
    for cp in metas + x_copies + t_copies + d_copies + r_copies:
        cp.wait_send()


def on_device(
    reference_act, codes, scale_index, scale_table, norm_gain, routes_fwd, probs_fwd,
    gate_weight, up_weight, down_weight, saved_input, routes_bwd, probs_bwd, saved_preact, cotangent,
):
    width, ffn = gate_weight.shape[2:]
    levels = scale_table.shape[0]
    picker = scale_index[0][:, None] == jnp.arange(levels, dtype=jnp.int32)[None, :]
    row_scale = jnp.sum(jnp.where(picker, scale_table[None, :], 0.0), axis=1, keepdims=True)
    routes = jnp.concatenate([routes_bwd[0], routes_fwd[0]], axis=0).astype(F32)
    probs = jnp.concatenate([probs_bwd[0], probs_fwd[0]], axis=0)
    meta = jnp.concatenate([routes, probs], axis=1).T
    slots = NX * CHUNK
    dma = pltpu.SemaphoreType.DMA
    anywhere = pl.BlockSpec(memory_space=pl.ANY)
    block = jax.ShapeDtypeStruct((ROWS, width), BF16)
    mixed, grad = pl.pallas_call(
        kernel,
        name="relay_moe",
        out_shape=(block, block),
        in_specs=[anywhere] * 11,
        out_specs=(pl.BlockSpec(memory_space=pltpu.VMEM),) * 2,
        scratch_shapes=[
            pltpu.VMEM((ROWS, width), BF16),
            pltpu.VMEM((ROWS, width), jnp.int32),
            pltpu.VMEM((ROWS, 1), F32),
            pltpu.VMEM((1, width), F32),
            pltpu.VMEM((ROWS, width), BF16),
            pltpu.VMEM((width, ffn), BF16),
            pltpu.VMEM((width, ffn), BF16),
            pltpu.VMEM((ffn, width), BF16),
            pltpu.VMEM((slots, 2 * ffn), BF16),
            pltpu.VMEM((ROWS, width), BF16),
            pltpu.VMEM((ROWS, width), BF16),
            pltpu.VMEM((ROWS, width), BF16),
            pltpu.VMEM((ROWS, width), BF16),
            pltpu.VMEM((ROWS, width), F32),
            pltpu.VMEM((16, 16, 128), F32),
            pltpu.VMEM((2, NX * NZ, 128), F32),
            pltpu.VMEM((2, NX * NZ, 128), F32),
            pltpu.VMEM((2, 16 * ROWS, width), BF16),
            pltpu.VMEM((2, 12 * SLOTS, width), BF16),
            pltpu.VMEM((2, slots, width), BF16),
            pltpu.VMEM((2, slots, width), BF16),
            pltpu.VMEM((2, NZ * ROWS, width), BF16),
            pltpu.VMEM((2, 7, ROWS, width), BF16),
            dma((10,)), dma((2,)), dma((2,)), dma((15,)), dma((15,)),
            dma((2, 7)), dma((2, 7)), dma((2, 8)), dma((2, 8)), dma((2, 12)), dma((2, 12)),
            dma((2, 12)), dma((2, 12)), dma((2, 8)), dma((2, 8)), dma((2, 7)), dma((2, 7)),
        ],
        compiler_params=pltpu.CompilerParams(
            collective_id=0, has_side_effects=True, vmem_limit_bytes=67_043_328
        ),
    )(
        reference_act[0], codes[0], row_scale, norm_gain, meta, saved_input[0], cotangent[0],
        gate_weight[0, 0], up_weight[0, 0], down_weight[0, 0], saved_preact[0, 0],
    )
    return mixed[None], grad[None]


def solution(mesh):
    grid = jax.sharding.Mesh(
        mesh.devices.reshape(4, NX, NZ, 2), ("section", "x", "z", "core")
    )
    tokens = ("x", "z", "core")
    return jax.shard_map(
        on_device,
        mesh=grid,
        in_specs=(
            P("section", tokens, None),
            P("section", tokens, None),
            P("section", tokens),
            P(),
            P("section", None),
            P("section", tokens, None),
            P("section", tokens, None),
            P("section", tokens, None, None),
            P("section", tokens, None, None),
            P("section", tokens, None, None),
            P("section", tokens, None),
            P("section", tokens, None),
            P("section", tokens, None),
            P("section", tokens, None, None),
            P("section", tokens, None),
        ),
        out_specs=(P("section", tokens, None), P("section", tokens, None)),
        check_vma=False,
    )
```

```python
import functools

import jax
import jax.numpy as jnp
from jax import lax
from jax.experimental import pallas as pl
from jax.experimental.pallas import tpu as pltpu
from jax.sharding import PartitionSpec as P

EPSILON = 1e-06
NX, NZ = 4, 8
ROWS = 64
CAP = 12
GROUP = 4
SLOTS = GROUP * CAP
TOKENS = GROUP * ROWS
CHUNK = 4 * SLOTS
COLS = 512
MESH = pl.DeviceIdType.MESH
F32, BF16 = jnp.float32, jnp.bfloat16


WIDTH = 2048
SIDE = 384
MAIN = WIDTH - SIDE
FIRST = ((0, 256), (256, 384), (640, 512), (1152, MAIN - 1152))
LAST = ((0, MAIN - 1152), (MAIN - 1152, 512), (MAIN - 640, 384), (MAIN - 256, 256))
WHOLE = ((0, MAIN),)
HALVES = ((0, 768), (768, MAIN - 768))
ZSLOTS = 8 * CAP
N_SENT, N_ARRIVED = 24, 136


def kernel(
    ref_h, codes_h, index_h, table_h, gain_h, rb_h, rf_h, pb_h, pf_h, saved_h, cot_h, gate_h, up_h, down_h, pre_h,
    out_o,
    ref_v, codes_v, index_v, table_v, gain_v, rb_v, rf_v, pb_v, pf_v, saved_v, gate_v, up_v, down_v, pre_v,
    dsend_v, drecv_v, gout_v, norm_v, inputs_v, meta_v, tgt_v, wgt_v, across_v, ztgt_v, zwgt_v, acc_v,
    ag, send, arr, ret, d2, rs, xg, zsend, zarr, zret, xd, xr, ld_s, snd, rcv,
):
    s, x, z, c = (lax.axis_index(a) for a in ("section", "x", "z", "core"))
    width = ref_v.shape[1]
    ffn = gate_v.shape[1]
    own = z * 2 + c
    sents, arrivals = {}, {}

    def at_z(off):
        return lax.rem(z + (off + NZ), NZ)

    def at_x(off):
        return lax.rem(x + off, NX)

    def rows_of(zz, cc):
        return pl.ds(pl.multiple_of((zz * 2 + cc) * ROWS, ROWS), ROWS)

    def remote(out, into, src, dst, dev):
        return pltpu.make_async_remote_copy(
            src_ref=src, dst_ref=dst,
            send_sem=snd.at[sents.setdefault(out, len(sents))],
            recv_sem=rcv.at[arrivals.setdefault(into, len(arrivals))],
            device_id=dev, device_id_type=MESH,
        )

    def put(out, into, src, dst, dev):
        remote(out, into, src, dst, dev).start()

    def arrived(into, like):
        remote("cot", into, like, like, {"core": 1 - c}).wait_recv()

    def sent(out, like):
        remote(out, "delta", like, like, {"core": 1 - c}).wait_send()

    names = ("rb", "rf", "pb", "pf", "codes", "index", "table", "ref", "gain", "saved", "down", "gate", "up", "pre")
    pairs = (
        (rb_h, rb_v), (rf_h, rf_v), (pb_h, pb_v), (pf_h, pf_v), (codes_h, codes_v), (index_h, index_v),
        (table_h, table_v), (ref_h, ref_v), (gain_h, gain_v), (saved_h, saved_v), (down_h, down_v),
        (gate_h, gate_v), (up_h, up_v), (pre_h, pre_v),
    )
    loads = {k: pltpu.make_async_copy(a, b, ld_s.at[n]) for n, (k, (a, b)) in enumerate(zip(names, pairs))}
    for ld in loads.values():
        ld.start()

    ahead, behind = {"section": lax.rem(s + 1, 4)}, {"section": lax.rem(s + 3, 4)}
    column = [(dz, dc) for dz in range(NZ) for dc in (0, 1) if (dz, dc) != (0, 0)]
    peers = [ahead, behind] + [{"x": at_x(d)} for d in (1, 2, 3)]
    peers += [{"z": at_z(dz), "core": lax.rem(c + dc, 2)} for dz, dc in column]
    peers += [{"x": at_x(d), "core": 1 - c} for d in (1, 2, 3)]
    row = [(dx, dc) for dx in range(NX) for dc in (0, 1) if (dx, dc) != (0, 0)]
    barrier = pltpu.get_barrier_semaphore()
    for dev in peers:
        pl.semaphore_signal(barrier, inc=1, device_id=dev, device_id_type=MESH)

    for k in names[:4]:
        loads[k].wait()
    eye_r = lax.broadcasted_iota(jnp.int32, (ROWS, 128), 0)
    eye_c = lax.broadcasted_iota(jnp.int32, (ROWS, 128), 1)
    low_eye = jnp.where(eye_c == eye_r, 1.0, 0.0)
    high_eye = jnp.where(eye_c == eye_r + ROWS, 1.0, 0.0)

    def side_by_side(low, high):
        one = jnp.dot(low.astype(F32), low_eye, precision=lax.Precision.HIGHEST)
        return one + jnp.dot(high.astype(F32), high_eye, precision=lax.Precision.HIGHEST)

    meta_v[own, 0:8, :] = side_by_side(rb_v[...], rf_v[...])
    meta_v[own, 8:16, :] = side_by_side(pb_v[...], pf_v[...])
    across_v[x * 2 + c] = meta_v[own]
    pl.semaphore_wait(barrier, len(peers))

    side = pl.ds(MAIN, SIDE)
    for q, (k0, w) in enumerate(FIRST[:1] + ((MAIN, SIDE),) + FIRST[1:]):
        put("cot", ("cot", k0), cot_h.at[:, pl.ds(k0, w)], gout_v.at[:, pl.ds(k0, w)], behind)
    for k, (dz, dc) in enumerate(column):
        put("meta", "meta", meta_v.at[own], meta_v.at[own], peers[5 + k])
    for k, (dx, dc) in enumerate(row):
        put(
            "across", "across", across_v.at[x * 2 + c], across_v.at[x * 2 + c],
            {"x": at_x(dx), "core": lax.rem(c + dc, 2)},
        )
    for k in ("codes", "index", "table"):
        loads[k].wait()
    levels = lax.broadcasted_iota(jnp.int32, (ROWS, 16), 1).astype(F32)
    square = lax.broadcasted_iota(jnp.int32, (ROWS, ROWS), 0) == lax.broadcasted_iota(jnp.int32, (ROWS, ROWS), 1)
    level = jnp.sum(jnp.where(square, index_v[...].astype(F32), 0.0), axis=1, keepdims=True)
    row_scale = jnp.sum(jnp.where(levels == level, table_v[...], 0.0), axis=1, keepdims=True)
    dsend_v[...] = (codes_v[...].astype(F32) * row_scale).astype(BF16)
    put("delta", "delta", dsend_v, drecv_v, ahead)

    chunks = (FIRST, HALVES)

    def hop(p, k, q, src):
        zz = at_z(1 - k) if k > 0 else at_z(-1 - k)
        cols = pl.ds(*chunks[p][q])
        put(("ring", p), ("ring", p, k, q), src.at[:, cols], ag.at[p, rows_of(zz, c), cols], {"z": at_z(1 if k > 0 else -1)})

    def to_sibling(p, k, q, src):
        cols = pl.ds(*chunks[p][q])
        put(("ring", p), ("sib", p, max(abs(k), 1), q), src.at[:, cols], ag.at[p, rows_of(at_z(-k), c), cols], {"core": 1 - c})

    def start_ring(p, q, src):
        cols = pl.ds(*chunks[p][q])
        hop(p, 1, q, src)
        hop(p, -1, q, src)
        to_sibling(p, 0, q, src)
        ag[p, rows_of(z, c), cols] = src[:, cols]

    def step(p, k, q):
        for j in (k, -k) if k < 4 else (k,):
            here = rows_of(at_z(-j), c)
            arrived(("ring", p, j, q), ag.at[p, here, pl.ds(*chunks[p][q])])
            if j not in (4, -3):
                hop(p, j + (1 if j > 0 else -1), q, ag.at[p, here])
            to_sibling(p, j, q, ag.at[p, here])

    def settle(p, k, q):
        count = {1: 3, 2: 2, 3: 2, 4: 1}[k]
        arrived(("sib", p, k, q), ag.at[p, pl.ds(0, count * ROWS), pl.ds(*chunks[p][q])])

    arrived(("cot", 0), gout_v.at[:, pl.ds(*FIRST[0])])
    start_ring(0, 0, gout_v)

    def spread(p, src):
        block = pl.ds(pl.multiple_of((x * 2 + c) * ROWS, ROWS), ROWS)
        for d in (1, 2, 3):
            put(("xg", p), ("xg", p), src.at[:, side], xg.at[p, block], {"x": at_x(d)})
        put(("xg", p), ("xs", p), src.at[:, side], xg.at[p, block], {"core": 1 - c})
        xg[p, block, :] = src[:, side]

    arrived(("cot", MAIN), gout_v.at[:, side])
    spread(0, gout_v)

    arrived("meta", meta_v.at[pl.ds(0, 15)])
    arrived("across", across_v.at[pl.ds(0, 7)])
    tri_r = lax.broadcasted_iota(jnp.int32, (128, 128), 0)
    tri_c = lax.broadcasted_iota(jnp.int32, (128, 128), 1)
    tri = jnp.where((tri_r < tri_c) & ((tri_r < ROWS) == (tri_c < ROWS)), 1.0, 0.0).astype(BF16)
    lane = lax.broadcasted_iota(jnp.int32, (32, 128), 1)
    line = lax.broadcasted_iota(jnp.int32, (32, 128), 0)
    core_shift = jnp.where(lane < ROWS, 0, CAP)
    shift = (core_shift + lax.rem(line, 2) * (2 * CAP)).astype(F32)
    zshift = (core_shift + (line // 8) * (2 * CAP)).astype(F32)

    def in_lanes(ref, pairs):
        flat = ref[...].reshape(pairs * 2 * 16, 128)
        turned = pltpu.roll(flat, ROWS, 1).reshape(pairs, 2, 16, 128)
        flat = flat.reshape(pairs, 2, 16, 128)
        low = lax.broadcasted_iota(jnp.int32, (pairs, 16, 128), 2) < ROWS
        first = jnp.where(low, flat[:, 0], turned[:, 1])
        second = jnp.where(low, turned[:, 0], flat[:, 1])
        return [(m[:, :8], m[:, 8:]) for m in (first, second)]

    def tables(p, hits, probs, shifts, tgt, wgt):
        named = jnp.concatenate([jnp.sum(jnp.where(h, 1.0, 0.0), axis=1) for h in hits], axis=0)
        earlier = jnp.dot(named.astype(BF16), tri, preferred_element_type=F32)
        tgt[p] = jnp.where(named > 0.5, earlier + shifts, -1.0)
        wgt[p] = jnp.concatenate(
            [jnp.sum(jnp.where(h, w, 0.0), axis=1) for h, w in zip(hits, probs)], axis=0
        )

    for p, (routes, probs) in enumerate(in_lanes(meta_v, NZ)):
        hits = [routes == (xe * 16 + own).astype(F32) for xe in range(NX)]
        tables(p, hits, [probs] * NX, shift, tgt_v, wgt_v)

    slot_iota = lax.broadcasted_iota(jnp.int32, (SLOTS, TOKENS), 0).astype(F32)

    def row_pair(ref, p, xe, g):
        at = xe * NZ + 2 * g
        return jnp.concatenate([ref[p, pl.ds(at, 1), :], ref[p, pl.ds(at + 1, 1), :]], axis=1)

    half = z // 2
    odd = 2 * lax.rem(z, 2) - 1
    order = [half, lax.rem(half + odd + 4, 4), lax.rem(half - odd + 4, 4), lax.rem(half + 2, 4)]

    def out_chunks(p, n):
        return FIRST if (p, n) == (0, 0) else WHOLE

    def picker(p, n):
        return jnp.concatenate(
            [jnp.where(slot_iota == row_pair(tgt_v, p, at_x(d), order[n]), 1.0, 0.0) for d in range(NX)], axis=0
        ).astype(BF16)

    def dispatch(p, n, q, pick):
        g = order[n]
        start, size = out_chunks(p, n)[q]
        here = pl.ds(pl.multiple_of(x * CHUNK + g * SLOTS, 16), SLOTS)
        for k in range(start, start + size, COLS):
            cols = pl.ds(k, min(COLS, start + size - k))
            block = ag[p, pl.ds(pl.multiple_of(g * TOKENS, TOKENS), TOKENS), cols]
            rows = jnp.dot(pick, block, preferred_element_type=F32).astype(BF16)
            arr[p, here, cols] = rows[:SLOTS]
            send[p, pl.ds(n * 3 * SLOTS, 3 * SLOTS), cols] = rows[SLOTS:]
        cols = pl.ds(start, size)
        for d in (1, 2, 3):
            put(
                ("x", p), ("x", p), send.at[p, pl.ds((n * 3 + d - 1) * SLOTS, SLOTS), cols],
                arr.at[p, here, cols], {"x": at_x(d)},
            )

    def relay(p):
        arrived(("xg", p), xr.at[p])
        for d in (1, 2, 3):
            block = pl.ds(pl.multiple_of((lax.rem(x - d + NX, NX) * 2 + c) * ROWS, ROWS), ROWS)
            put(("xg", p), ("xs", p), xg.at[p, block], xg.at[p, block], {"core": 1 - c})

    zslot_iota = lax.broadcasted_iota(jnp.int32, (ZSLOTS, 128), 0).astype(F32)

    def zslots(p):
        arrived(("xs", p), xd.at[p])
        here = pl.ds(pl.multiple_of(z * ZSLOTS, ZSLOTS), ZSLOTS)
        for dz in range(NZ):
            pick = jnp.concatenate(
                [
                    jnp.where(zslot_iota == ztgt_v[p, pl.ds(xs * NZ + at_z(dz), 1), :], 1.0, 0.0)
                    for xs in range(NX)
                ],
                axis=1,
            ).astype(BF16)
            rows = jnp.dot(pick, xg[p], preferred_element_type=F32).astype(BF16)
            if dz == 0:
                zarr[p, here, :] = rows
            else:
                zsend[p, (dz - 1) * ZSLOTS : dz * ZSLOTS, :] = rows

    def zpush(p, some):
        here = pl.ds(pl.multiple_of(z * ZSLOTS, ZSLOTS), ZSLOTS)
        for dz in some:
            put(
                ("zs", p), ("zs", p), zsend.at[p, pl.ds((dz - 1) * ZSLOTS, ZSLOTS)], zarr.at[p, here],
                {"z": at_z(dz)},
            )

    def in_order(p, k):
        r = lax.broadcasted_iota(jnp.int32, (CHUNK, NX * CHUNK), 0)
        m = lax.broadcasted_iota(jnp.int32, (CHUNK, NX * CHUNK), 1)
        want = r + k * (2 * CAP)
        for j in range(1, NZ):
            want += jnp.where(r >= j * 2 * CAP, ZSLOTS - 2 * CAP, 0)
        pick = jnp.where(m == want, 1.0, 0.0).astype(BF16)
        return jnp.dot(pick, zarr[p], preferred_element_type=F32).astype(BF16)

    def out_of_order(p):
        @pl.loop(0, NX)
        def _(k):
            m = lax.broadcasted_iota(jnp.int32, (CHUNK, NX * CHUNK), 0)
            r = lax.broadcasted_iota(jnp.int32, (CHUNK, NX * CHUNK), 1)
            upper = m >= ZSLOTS
            within = m - jnp.where(upper, ZSLOTS, 0)
            want = within + (2 * k + jnp.where(upper, 1, 0)) * (2 * CAP)
            for j in range(1, NX):
                want += jnp.where(within >= j * 2 * CAP, CHUNK - 2 * CAP, 0)
            pick = jnp.where(r == want, 1.0, 0.0).astype(BF16)
            rows = jnp.dot(pick, arr[p, :, MAIN:], preferred_element_type=F32)
            zarr[p, pl.ds(pl.multiple_of(k * CHUNK, CHUNK), CHUNK), :] = rows.astype(BF16)

    def zback(p, some):
        here = pl.ds(pl.multiple_of(z * ZSLOTS, ZSLOTS), ZSLOTS)
        for dz in some:
            there = pl.ds(pl.multiple_of(at_z(dz) * ZSLOTS, ZSLOTS), ZSLOTS)
            put(("zt", p), ("zt", p), zarr.at[p, there], zret.at[p, here], {"z": at_z(dz)})

    def zcombine(p):
        mine = pl.ds(pl.multiple_of(z * ZSLOTS, ZSLOTS), ZSLOTS)
        zret[p, mine, :] = zarr[p, mine, :]
        arrived(("zt", p), zsend.at[p])
        for xs in range(NX):
            share = jnp.concatenate(
                [
                    jnp.where(
                        zslot_iota == ztgt_v[p, pl.ds(xs * NZ + ze, 1), :], zwgt_v[p, pl.ds(xs * NZ + ze, 1), :], 0.0
                    )
                    for ze in range(NZ)
                ],
                axis=0,
            ).T.astype(BF16)
            got = jnp.dot(share, zret[p], preferred_element_type=F32)
            xg[p, xs * 128 : (xs + 1) * 128, :] = got.astype(BF16)
        for xs in range(NX):
            away = pl.ds(pl.multiple_of(xs * 128 + (1 - c) * ROWS, ROWS), ROWS)
            put(("xd", p), ("xd", p), xg.at[p, away], xd.at[p, pl.ds(xs * ROWS, ROWS)], {"core": 1 - c})
        arrived(("xd", p), xd.at[p])
        for xs in range(NX):
            land = pl.ds(xs * ROWS, ROWS)
            stay = pl.ds(pl.multiple_of(xs * 128 + c * ROWS, ROWS), ROWS)
            xg[p, stay, :] = (xg[p, stay, :].astype(F32) + xd[p, land, :].astype(F32)).astype(BF16)
        for d in (2, 1, 3):
            block = pl.ds(pl.multiple_of((at_x(d) * 2 + c) * ROWS, ROWS), ROWS)
            put(("xr", p), ("xr", p), xg.at[p, block], xr.at[p, d - 1], {"x": at_x(d)})

    def zowned(p):
        total = xg[p, pl.ds(pl.multiple_of((x * 2 + c) * ROWS, ROWS), ROWS), :].astype(F32)
        arrived(("xr", p), xr.at[p])
        for d in (1, 2, 3):
            total += xr[p, d - 1].astype(F32)
        return total

    for q in range(1, len(FIRST)):
        arrived(("cot", FIRST[q][0]), gout_v.at[:, pl.ds(*FIRST[q])])
        start_ring(0, q, gout_v)
    pick = picker(0, 0)
    for q in range(len(FIRST)):
        step(0, 1, q)
        settle(0, 1, q)
        dispatch(0, 0, q, pick)

    relay(0)

    arrived("delta", drecv_v)
    loads["ref"].wait()
    loads["gain"].wait()
    inputs = ref_v[...].astype(F32) + drecv_v[...].astype(F32) * jnp.where(s > 0, 1.0, 0.0)
    inputs_v[...] = inputs
    inverse = lax.rsqrt(jnp.mean(inputs * inputs, axis=-1, keepdims=True) + EPSILON)
    norm_v[...] = (inputs * inverse * gain_v[...]).astype(BF16)

    for p, (routes, probs) in enumerate(in_lanes(across_v, NX)):
        expert = (lax.broadcasted_iota(jnp.int32, (NZ, 8, 128), 0) * 2 + x * 16 + c).astype(F32)
        hits = [routes[xs][None] == expert for xs in range(NX)]
        tables(p, hits, [probs[xs][None] for xs in range(NX)], zshift, ztgt_v, zwgt_v)

    for n in (1, 2, 3):
        for q in range(len(FIRST)):
            step(0, n + 1, q)
        if n == 2:
            for q in range(len(HALVES)):
                start_ring(1, q, norm_v)
            spread(1, norm_v)
        for q in range(len(FIRST)):
            settle(0, n + 1, q)
        dispatch(0, n, 0, picker(0, n))
    zslots(0)
    for n in range(4):
        for q in range(len(HALVES)):
            step(1, n + 1, q)
        zpush(0, ((1, 7), (2, 6), (3, 5), (4,))[n])
        for q in range(len(HALVES)):
            settle(1, n + 1, q)
        dispatch(1, n, 0, picker(1, n))
        if n == 0:
            relay(1)
        if n == 2:
            zslots(1)
    zpush(1, (4, 3, 5, 2, 6, 1, 7))

    def slots_arrived(p):
        arrived(("x", p), send.at[p])
        arrived(("zs", p), zsend.at[p])

    across = (((1,), (1,)), ((), ()))

    slots_arrived(0)
    for k in names[9:]:
        loads[k].wait()

    @pl.loop(0, NX)
    def _(k):
        at = pl.ds(pl.multiple_of(k * CHUNK, CHUNK), CHUNK)
        arr[0, at, MAIN:] = in_order(0, k)
        hidden = lax.dot_general(arr[0, at, :], down_v[...], across, preferred_element_type=F32)
        gate_act = pre_v[at, :ffn].astype(F32)
        up_act = pre_v[at, ffn:].astype(F32)
        sigma = jax.nn.sigmoid(gate_act)
        grad_gate = (hidden * up_act * sigma * (1.0 + gate_act * (1.0 - sigma))).astype(BF16)
        grad_up = (hidden * gate_act * sigma).astype(BF16)
        for j in range(0, width, COLS):
            total = lax.dot_general(grad_gate, gate_v[j : j + COLS, :], across, preferred_element_type=F32)
            total += lax.dot_general(grad_up, up_v[j : j + COLS, :], across, preferred_element_type=F32)
            arr[0, at, j : j + COLS] = total.astype(BF16)

    def back_chunks(p, n):
        return LAST if (p, n) == (1, 3) else WHOLE

    def give_back(p, some):
        for n in some:
            g = order[3 - n]
            for q, cols in enumerate(back_chunks(p, n)):
                cols = pl.ds(*cols)
                for d in (1, 2, 3):
                    where = pl.ds(pl.multiple_of(at_x(d) * CHUNK + g * SLOTS, 16), SLOTS)
                    land = pl.ds(pl.multiple_of(n * CHUNK + x * SLOTS, 16), SLOTS)
                    put(("t", p), ("t", p, n, q), arr.at[p, where, cols], ret.at[p, land, cols], {"x": at_x(d)})

    out_of_order(0)
    give_back(0, (0, 1, 2, 3))
    zback(0, (4, 3, 5, 2, 6, 1, 7))

    slots_arrived(1)

    @pl.loop(0, NX)
    def _(k):
        at = pl.ds(pl.multiple_of(k * CHUNK, CHUNK), CHUNK)
        arr[1, at, MAIN:] = in_order(1, k)
        rows = arr[1, at, :]
        gate_act = jnp.dot(rows, gate_v[...], preferred_element_type=F32)
        up_act = jnp.dot(rows, up_v[...], preferred_element_type=F32)
        hidden = (gate_act * jax.nn.sigmoid(gate_act) * up_act).astype(BF16)
        for j in range(0, width, COLS):
            total = jnp.dot(hidden, down_v[:, j : j + COLS], preferred_element_type=F32)
            arr[1, at, j : j + COLS] = total.astype(BF16)

    out_of_order(1)
    give_back(1, (0, 1, 2))

    for p in (0, 1):
        sent(("ring", p), ag.at[p, pl.ds(0, 15 * ROWS)])
        sent(("xg", p), xg.at[p, pl.ds(0, 7 * ROWS)])

    def shares(p, n):
        g = order[3 - n]
        return jnp.concatenate(
            [
                jnp.where(slot_iota == row_pair(tgt_v, p, xe, g), row_pair(wgt_v, p, xe, g), 0.0)
                for xe in range(NX)
            ],
            axis=0,
        ).T.astype(BF16)

    def combine(p, n, q, share):
        g = order[3 - n]
        start, size = back_chunks(p, n)[q]
        part = pl.ds(start, size)
        arrived(("t", p, n, q), ret.at[p, pl.ds(n * CHUNK, 3 * SLOTS), part])
        mine = pl.ds(pl.multiple_of(n * CHUNK + x * SLOTS, 16), SLOTS)
        here = pl.ds(pl.multiple_of(x * CHUNK + g * SLOTS, 16), SLOTS)
        ret[p, mine, part] = arr[p, here, part]
        tokens = pl.ds(pl.multiple_of(g * TOKENS, TOKENS), TOKENS)
        for k in range(start, start + size, COLS):
            cols = pl.ds(k, min(COLS, start + size - k))
            got = jnp.dot(share, ret[p, pl.ds(n * CHUNK, CHUNK), cols], preferred_element_type=F32)
            ag[p, tokens, cols] = got.astype(BF16)
        for h in (0, 1):
            away = pl.ds(pl.multiple_of(g * TOKENS + h * 128 + (1 - c) * ROWS, ROWS), ROWS)
            put(
                ("d", p), ("d", p, n, q), ag.at[p, away, part], d2.at[p, pl.ds((n * 2 + h) * ROWS, ROWS), part],
                {"core": 1 - c},
            )
        arrived(("d", p, n, q), d2.at[p, pl.ds(n * 2 * ROWS, 2 * ROWS), part])
        for h in (0, 1):
            land = pl.ds((n * 2 + h) * ROWS, ROWS)
            stay = pl.ds(pl.multiple_of(g * TOKENS + h * 128 + c * ROWS, ROWS), ROWS)
            ag[p, stay, part] = (ag[p, stay, part].astype(F32) + d2[p, land, part].astype(F32)).astype(BF16)

    def place(k):
        return k - 1 if k > 0 else 3 - k

    def pass_chunks(p, k):
        return back_chunks(p, 3) if k in (3, 4, -2, -3) else WHOLE

    def pass_on(p, k, q=0):
        there = rows_of(at_z(5 - k) if k > 0 else at_z(-4 - k), c)
        part = pl.ds(*pass_chunks(p, k)[q])
        if k not in (1, -1):
            last = k - 1 if k > 0 else k + 1
            split = pass_chunks(p, last)
            if q < len(split):
                arrived(("r", p, last, q), rs.at[p, place(last), :, pl.ds(*split[q])])
            ag[p, there, part] = (ag[p, there, part].astype(F32) + rs[p, place(last), :, part].astype(F32)).astype(BF16)
        put(("r", p), ("r", p, k, q), ag.at[p, there, part], rs.at[p, place(k), :, part], {"z": at_z(1 if k > 0 else -1)})

    def owned(p, q):
        part = pl.ds(*back_chunks(p, 3)[q])
        for k in (4, -3):
            arrived(("r", p, k, q), rs.at[p, place(k), :, part])
        total = ag[p, rows_of(z, c), part].astype(F32)
        return total + rs[p, place(4), :, part].astype(F32) + rs[p, place(-3), :, part].astype(F32)

    def pass_pair(p, k):
        for q in range(len(pass_chunks(p, k))):
            pass_on(p, 1 - k, q)
            pass_on(p, k, q)

    combine(0, 0, 0, shares(0, 0))
    pass_on(0, 1)
    zback(1, (1, 7))
    combine(0, 1, 0, shares(0, 1))
    pass_on(0, -1)
    zback(1, (2, 6))
    zcombine(0)
    give_back(1, (3,))
    combine(0, 2, 0, shares(0, 2))
    pass_on(0, 2)
    zback(1, (3, 5))
    combine(0, 3, 0, shares(0, 3))
    pass_pair(0, 3)
    zback(1, (4,))
    combine(1, 0, 0, shares(1, 0))
    pass_on(1, 1)
    pass_pair(0, 4)
    combine(1, 1, 0, shares(1, 1))
    pass_on(1, -1)
    pass_on(1, 2)
    combine(1, 2, 0, shares(1, 2))
    pass_pair(1, 3)
    zcombine(1)

    acc_v[:, :MAIN] = owned(0, 0)
    acc_v[:, MAIN:] = zowned(0)
    weighted = acc_v[...] * gain_v[...]
    saved = saved_v[...].astype(F32)
    scale = lax.rsqrt(jnp.mean(saved * saved, axis=-1, keepdims=True) + EPSILON)
    projection = jnp.mean(weighted * saved, axis=-1, keepdims=True)
    out_o[1] = (
        gout_v[...].astype(F32) + scale * weighted - saved * (scale * scale * scale * projection)
    ).astype(BF16)

    share = shares(1, 3)
    for q in range(len(LAST)):
        combine(1, 3, q, share)
        pass_on(1, -3, q)
        pass_on(1, 4, q)
    for q, cols in enumerate(LAST):
        cols = pl.ds(*cols)
        out_o[0, :, cols] = (inputs_v[:, cols] + owned(1, q)).astype(BF16)
    out_o[0, :, MAIN:] = (inputs_v[:, MAIN:] + zowned(1)).astype(BF16)

    sent("cot", gout_v)
    sent("delta", dsend_v)
    sent("meta", meta_v.at[pl.ds(0, 15)])
    sent("across", across_v.at[pl.ds(0, 7)])
    for p in (0, 1):
        for kind, like in (
            ("x", send), ("t", send), ("zs", zsend), ("zt", zsend), ("d", d2), ("r", rs), ("xd", xd), ("xr", xr),
        ):
            sent((kind, p), like.at[p])
    assert (len(sents), len(arrivals)) == (N_SENT, N_ARRIVED), (len(sents), len(arrivals))


def on_device(
    reference_act, codes, scale_index, scale_table, norm_gain, routes_fwd, probs_fwd,
    gate_weight, up_weight, down_weight, saved_input, routes_bwd, probs_bwd, saved_preact, cotangent,
):
    width, ffn = gate_weight.shape[2:]
    slots = NX * CHUNK
    dma = pltpu.SemaphoreType.DMA
    both = pl.pallas_call(
        kernel,
        name="relay_moe",
        out_shape=jax.ShapeDtypeStruct((2, ROWS, width), BF16),
        in_specs=[pl.BlockSpec(memory_space=pl.ANY)] * 15,
        out_specs=pl.BlockSpec(memory_space=pltpu.VMEM),
        scratch_shapes=[
            pltpu.VMEM((ROWS, width), BF16),
            pltpu.VMEM((ROWS, width), jnp.int32),
            pltpu.VMEM((1, ROWS), jnp.int32),
            pltpu.VMEM((1, 16), F32),
            pltpu.VMEM((1, width), F32),
            pltpu.VMEM((8, ROWS), jnp.int32),
            pltpu.VMEM((8, ROWS), jnp.int32),
            pltpu.VMEM((8, ROWS), F32),
            pltpu.VMEM((8, ROWS), F32),
            pltpu.VMEM((ROWS, width), BF16),
            pltpu.VMEM((width, ffn), BF16),
            pltpu.VMEM((width, ffn), BF16),
            pltpu.VMEM((ffn, width), BF16),
            pltpu.VMEM((slots, 2 * ffn), BF16),
            pltpu.VMEM((ROWS, width), BF16),
            pltpu.VMEM((ROWS, width), BF16),
            pltpu.VMEM((ROWS, width), BF16),
            pltpu.VMEM((ROWS, width), BF16),
            pltpu.VMEM((ROWS, width), F32),
            pltpu.VMEM((16, 16, 128), F32),
            pltpu.VMEM((2, NX * NZ, 128), F32),
            pltpu.VMEM((2, NX * NZ, 128), F32),
            pltpu.VMEM((8, 16, 128), F32),
            pltpu.VMEM((2, NX * NZ, 128), F32),
            pltpu.VMEM((2, NX * NZ, 128), F32),
            pltpu.VMEM((ROWS, width), F32),
            pltpu.VMEM((2, 16 * ROWS, MAIN), BF16),
            pltpu.VMEM((2, 12 * SLOTS, MAIN), BF16),
            pltpu.VMEM((2, slots, width), BF16),
            pltpu.VMEM((2, slots, MAIN), BF16),
            pltpu.VMEM((2, NZ * ROWS, MAIN), BF16),
            pltpu.VMEM((2, 7, ROWS, MAIN), BF16),
            pltpu.VMEM((2, 8 * ROWS, SIDE), BF16),
            pltpu.VMEM((2, 7 * ZSLOTS, SIDE), BF16),
            pltpu.VMEM((2, NZ * ZSLOTS, SIDE), BF16),
            pltpu.VMEM((2, NZ * ZSLOTS, SIDE), BF16),
            pltpu.VMEM((2, NX * ROWS, SIDE), BF16),
            pltpu.VMEM((2, 3, ROWS, SIDE), BF16),
            dma((14,)), dma((N_SENT,)), dma((N_ARRIVED,)),
        ],
        compiler_params=pltpu.CompilerParams(
            collective_id=0, has_side_effects=True, vmem_limit_bytes=67_043_328
        ),
    )(
        reference_act[0], codes[0], scale_index, scale_table[None], norm_gain,
        routes_bwd[0].T, routes_fwd[0].T, probs_bwd[0].T, probs_fwd[0].T, saved_input[0], cotangent[0],
        gate_weight[0, 0], up_weight[0, 0], down_weight[0, 0], saved_preact[0, 0],
    )
    return both[0:1], both[1:2]


def solution(mesh):
    grid = jax.sharding.Mesh(
        mesh.devices.reshape(4, NX, NZ, 2), ("section", "x", "z", "core")
    )
    tokens = ("x", "z", "core")
    return jax.shard_map(
        on_device,
        mesh=grid,
        in_specs=(
            P("section", tokens, None),
            P("section", tokens, None),
            P("section", tokens),
            P(),
            P("section", None),
            P("section", tokens, None),
            P("section", tokens, None),
            P("section", tokens, None, None),
            P("section", tokens, None, None),
            P("section", tokens, None, None),
            P("section", tokens, None),
            P("section", tokens, None),
            P("section", tokens, None),
            P("section", tokens, None, None),
            P("section", tokens, None),
        ),
        out_specs=(P("section", tokens, None), P("section", tokens, None)),
        check_vma=False,
    )
```

```python
import functools

import jax
import jax.numpy as jnp
from jax import lax
from jax.experimental import pallas as pl
from jax.experimental.pallas import tpu as pltpu
from jax.sharding import PartitionSpec as P

EPSILON = 1e-06
NX, NZ = 4, 8
ROWS = 64
CAP = 12
GROUP = 4
SLOTS = GROUP * CAP
TOKENS = GROUP * ROWS
CHUNK = 4 * SLOTS
COLS = 512
MESH = pl.DeviceIdType.MESH
F32, BF16 = jnp.float32, jnp.bfloat16


WIDTH = 2048
SIDE = 384
MAIN = WIDTH - SIDE
FIRST = ((0, 256), (256, 384), (640, 512), (1152, MAIN - 1152))
LAST = ((0, MAIN - 1152), (MAIN - 1152, 512), (MAIN - 640, 384), (MAIN - 256, 256))
WHOLE = ((0, MAIN),)
HALVES = ((0, 768), (768, MAIN - 768))
ZSLOTS = 8 * CAP
N_SENT, N_ARRIVED = 24, 136


def kernel(
    ref_h, codes_h, index_h, table_h, gain_h, rb_h, rf_h, pb_h, pf_h, saved_h, cot_h, gate_h, up_h, down_h, pre_h,
    out_o,
    ref_v, codes_v, index_v, table_v, gain_v, rb_v, rf_v, pb_v, pf_v, saved_v, gate_v, up_v, down_v, pre_v,
    dsend_v, drecv_v, gout_v, norm_v, inputs_v, meta_v, tgt_v, wgt_v, across_v, ztgt_v, zwgt_v, acc_v,
    ag, send, arr, ret, d2, rs, xg, zsend, zarr, zret, xd, xr, ld_s, snd, rcv,
):
    s, x, z, c = (lax.axis_index(a) for a in ("section", "x", "z", "core"))
    width = ref_v.shape[1]
    ffn = gate_v.shape[1]
    own = z * 2 + c
    sents, arrivals = {}, {}

    def at_z(off):
        return lax.rem(z + (off + NZ), NZ)

    def at_x(off):
        return lax.rem(x + off, NX)

    def rows_of(zz, cc):
        return pl.ds(pl.multiple_of((zz * 2 + cc) * ROWS, ROWS), ROWS)

    def remote(out, into, src, dst, dev):
        return pltpu.make_async_remote_copy(
            src_ref=src, dst_ref=dst,
            send_sem=snd.at[sents.setdefault(out, len(sents))],
            recv_sem=rcv.at[arrivals.setdefault(into, len(arrivals))],
            device_id=dev, device_id_type=MESH,
        )

    def put(out, into, src, dst, dev):
        remote(out, into, src, dst, dev).start()

    def arrived(into, like):
        remote("cot", into, like, like, {"core": 1 - c}).wait_recv()

    def sent(out, like):
        remote(out, "delta", like, like, {"core": 1 - c}).wait_send()

    names = ("rb", "rf", "pb", "pf", "codes", "index", "table", "ref", "gain", "saved", "down", "gate", "up", "pre")
    pairs = (
        (rb_h, rb_v), (rf_h, rf_v), (pb_h, pb_v), (pf_h, pf_v), (codes_h, codes_v), (index_h, index_v),
        (table_h, table_v), (ref_h, ref_v), (gain_h, gain_v), (saved_h, saved_v), (down_h, down_v),
        (gate_h, gate_v), (up_h, up_v), (pre_h, pre_v),
    )
    loads = {k: pltpu.make_async_copy(a, b, ld_s.at[n]) for n, (k, (a, b)) in enumerate(zip(names, pairs))}
    for ld in loads.values():
        ld.start()

    ahead, behind = {"section": lax.rem(s + 1, 4)}, {"section": lax.rem(s + 3, 4)}
    column = [(dz, dc) for dz in range(NZ) for dc in (0, 1) if (dz, dc) != (0, 0)]
    peers = [ahead, behind] + [{"x": at_x(d)} for d in (1, 2, 3)]
    peers += [{"z": at_z(dz), "core": lax.rem(c + dc, 2)} for dz, dc in column]
    peers += [{"x": at_x(d), "core": 1 - c} for d in (1, 2, 3)]
    row = [(dx, dc) for dx in range(NX) for dc in (0, 1) if (dx, dc) != (0, 0)]
    barrier = pltpu.get_barrier_semaphore()
    for dev in peers:
        pl.semaphore_signal(barrier, inc=1, device_id=dev, device_id_type=MESH)

    for k in names[:4]:
        loads[k].wait()
    eye_r = lax.broadcasted_iota(jnp.int32, (ROWS, 128), 0)
    eye_c = lax.broadcasted_iota(jnp.int32, (ROWS, 128), 1)
    low_eye = jnp.where(eye_c == eye_r, 1.0, 0.0)
    high_eye = jnp.where(eye_c == eye_r + ROWS, 1.0, 0.0)

    def side_by_side(low, high):
        one = jnp.dot(low.astype(F32), low_eye, precision=lax.Precision.HIGHEST)
        return one + jnp.dot(high.astype(F32), high_eye, precision=lax.Precision.HIGHEST)

    meta_v[own, 0:8, :] = side_by_side(rb_v[...], rf_v[...])
    meta_v[own, 8:16, :] = side_by_side(pb_v[...], pf_v[...])
    across_v[x * 2 + c] = meta_v[own]
    pl.semaphore_wait(barrier, len(peers))

    side = pl.ds(MAIN, SIDE)
    for q, (k0, w) in enumerate(FIRST[:1] + ((MAIN, SIDE),) + FIRST[1:]):
        put("cot", ("cot", k0), cot_h.at[:, pl.ds(k0, w)], gout_v.at[:, pl.ds(k0, w)], behind)
    for k, (dz, dc) in enumerate(column):
        put("meta", "meta", meta_v.at[own], meta_v.at[own], peers[5 + k])
    for k, (dx, dc) in enumerate(row):
        put(
            "across", "across", across_v.at[x * 2 + c], across_v.at[x * 2 + c],
            {"x": at_x(dx), "core": lax.rem(c + dc, 2)},
        )
    for k in ("codes", "index", "table"):
        loads[k].wait()
    levels = lax.broadcasted_iota(jnp.int32, (ROWS, 16), 1).astype(F32)
    square = lax.broadcasted_iota(jnp.int32, (ROWS, ROWS), 0) == lax.broadcasted_iota(jnp.int32, (ROWS, ROWS), 1)
    level = jnp.sum(jnp.where(square, index_v[...].astype(F32), 0.0), axis=1, keepdims=True)
    row_scale = jnp.sum(jnp.where(levels == level, table_v[...], 0.0), axis=1, keepdims=True)
    dsend_v[...] = (codes_v[...].astype(F32) * row_scale).astype(BF16)
    put("delta", "delta", dsend_v, drecv_v, ahead)

    chunks = (FIRST, HALVES)

    def hop(p, k, q, src):
        zz = at_z(1 - k) if k > 0 else at_z(-1 - k)
        cols = pl.ds(*chunks[p][q])
        put(("ring", p), ("ring", p, k, q), src.at[:, cols], ag.at[p, rows_of(zz, c), cols], {"z": at_z(1 if k > 0 else -1)})

    def to_sibling(p, k, q, src):
        cols = pl.ds(*chunks[p][q])
        put(("ring", p), ("sib", p, max(abs(k), 1), q), src.at[:, cols], ag.at[p, rows_of(at_z(-k), c), cols], {"core": 1 - c})

    def start_ring(p, q, src):
        cols = pl.ds(*chunks[p][q])
        hop(p, 1, q, src)
        hop(p, -1, q, src)
        to_sibling(p, 0, q, src)
        ag[p, rows_of(z, c), cols] = src[:, cols]

    def step(p, k, q):
        for j in (k, -k) if k < 4 else (k,):
            here = rows_of(at_z(-j), c)
            arrived(("ring", p, j, q), ag.at[p, here, pl.ds(*chunks[p][q])])
            if j not in (4, -3):
                hop(p, j + (1 if j > 0 else -1), q, ag.at[p, here])
            to_sibling(p, j, q, ag.at[p, here])

    def settle(p, k, q):
        count = {1: 3, 2: 2, 3: 2, 4: 1}[k]
        arrived(("sib", p, k, q), ag.at[p, pl.ds(0, count * ROWS), pl.ds(*chunks[p][q])])

    arrived(("cot", 0), gout_v.at[:, pl.ds(*FIRST[0])])
    start_ring(0, 0, gout_v)

    def spread(p, src):
        block = pl.ds(pl.multiple_of((x * 2 + c) * ROWS, ROWS), ROWS)
        for d in (1, 2, 3):
            put(("xg", p), ("xg", p), src.at[:, side], xg.at[p, block], {"x": at_x(d)})
        put(("xg", p), ("xs", p), src.at[:, side], xg.at[p, block], {"core": 1 - c})
        xg[p, block, :] = src[:, side]

    arrived(("cot", MAIN), gout_v.at[:, side])
    spread(0, gout_v)

    arrived("meta", meta_v.at[pl.ds(0, 15)])
    arrived("across", across_v.at[pl.ds(0, 7)])
    tri_r = lax.broadcasted_iota(jnp.int32, (128, 128), 0)
    tri_c = lax.broadcasted_iota(jnp.int32, (128, 128), 1)
    tri = jnp.where((tri_r < tri_c) & ((tri_r < ROWS) == (tri_c < ROWS)), 1.0, 0.0).astype(BF16)
    lane = lax.broadcasted_iota(jnp.int32, (32, 128), 1)
    line = lax.broadcasted_iota(jnp.int32, (32, 128), 0)
    core_shift = jnp.where(lane < ROWS, 0, CAP)
    shift = (core_shift + lax.rem(line, 2) * (2 * CAP)).astype(F32)
    zshift = (core_shift + (line // 8) * (2 * CAP)).astype(F32)

    def in_lanes(ref, pairs):
        flat = ref[...].reshape(pairs * 2 * 16, 128)
        turned = pltpu.roll(flat, ROWS, 1).reshape(pairs, 2, 16, 128)
        flat = flat.reshape(pairs, 2, 16, 128)
        low = lax.broadcasted_iota(jnp.int32, (pairs, 16, 128), 2) < ROWS
        first = jnp.where(low, flat[:, 0], turned[:, 1])
        second = jnp.where(low, turned[:, 0], flat[:, 1])
        return [(m[:, :8], m[:, 8:]) for m in (first, second)]

    def tables(p, hits, probs, shifts, tgt, wgt):
        named = jnp.concatenate([jnp.sum(jnp.where(h, 1.0, 0.0), axis=1) for h in hits], axis=0)
        earlier = jnp.dot(named.astype(BF16), tri, preferred_element_type=F32)
        tgt[p] = jnp.where(named > 0.5, earlier + shifts, -1.0)
        wgt[p] = jnp.concatenate(
            [jnp.sum(jnp.where(h, w, 0.0), axis=1) for h, w in zip(hits, probs)], axis=0
        )

    for p, (routes, probs) in enumerate(in_lanes(meta_v, NZ)):
        hits = [routes == (xe * 16 + own).astype(F32) for xe in range(NX)]
        tables(p, hits, [probs] * NX, shift, tgt_v, wgt_v)

    slot_iota = lax.broadcasted_iota(jnp.int32, (SLOTS, TOKENS), 0).astype(F32)

    def row_pair(ref, p, xe, g):
        at = xe * NZ + 2 * g
        return jnp.concatenate([ref[p, pl.ds(at, 1), :], ref[p, pl.ds(at + 1, 1), :]], axis=1)

    half = z // 2
    odd = 2 * lax.rem(z, 2) - 1
    order = [half, lax.rem(half + odd + 4, 4), lax.rem(half - odd + 4, 4), lax.rem(half + 2, 4)]

    def out_chunks(p, n):
        return FIRST if (p, n) == (0, 0) else WHOLE

    def picker(p, n):
        return jnp.concatenate(
            [jnp.where(slot_iota == row_pair(tgt_v, p, at_x(d), order[n]), 1.0, 0.0) for d in range(NX)], axis=0
        ).astype(BF16)

    def dispatch(p, n, q, pick):
        g = order[n]
        start, size = out_chunks(p, n)[q]
        here = pl.ds(pl.multiple_of(x * CHUNK + g * SLOTS, 16), SLOTS)
        for k in range(start, start + size, COLS):
            cols = pl.ds(k, min(COLS, start + size - k))
            block = ag[p, pl.ds(pl.multiple_of(g * TOKENS, TOKENS), TOKENS), cols]
            rows = jnp.dot(pick, block, preferred_element_type=F32).astype(BF16)
            arr[p, here, cols] = rows[:SLOTS]
            send[p, pl.ds(n * 3 * SLOTS, 3 * SLOTS), cols] = rows[SLOTS:]
        cols = pl.ds(start, size)
        for d in (1, 2, 3):
            put(
                ("x", p), ("x", p), send.at[p, pl.ds((n * 3 + d - 1) * SLOTS, SLOTS), cols],
                arr.at[p, here, cols], {"x": at_x(d)},
            )

    def relay(p):
        arrived(("xg", p), xr.at[p])
        for d in (1, 2, 3):
            block = pl.ds(pl.multiple_of((lax.rem(x - d + NX, NX) * 2 + c) * ROWS, ROWS), ROWS)
            put(("xg", p), ("xs", p), xg.at[p, block], xg.at[p, block], {"core": 1 - c})

    zslot_iota = lax.broadcasted_iota(jnp.int32, (ZSLOTS, 128), 0).astype(F32)

    def zslots(p):
        arrived(("xs", p), xd.at[p])
        here = pl.ds(pl.multiple_of(z * ZSLOTS, ZSLOTS), ZSLOTS)
        for dz in range(NZ):
            pick = jnp.concatenate(
                [
                    jnp.where(zslot_iota == ztgt_v[p, pl.ds(xs * NZ + at_z(dz), 1), :], 1.0, 0.0)
                    for xs in range(NX)
                ],
                axis=1,
            ).astype(BF16)
            rows = jnp.dot(pick, xg[p], preferred_element_type=F32).astype(BF16)
            if dz == 0:
                zarr[p, here, :] = rows
            else:
                zsend[p, (dz - 1) * ZSLOTS : dz * ZSLOTS, :] = rows

    def zpush(p, some):
        here = pl.ds(pl.multiple_of(z * ZSLOTS, ZSLOTS), ZSLOTS)
        for dz in some:
            put(
                ("zs", p), ("zs", p), zsend.at[p, pl.ds((dz - 1) * ZSLOTS, ZSLOTS)], zarr.at[p, here],
                {"z": at_z(dz)},
            )

    def in_order(p, k):
        r = lax.broadcasted_iota(jnp.int32, (CHUNK, NX * CHUNK), 0)
        m = lax.broadcasted_iota(jnp.int32, (CHUNK, NX * CHUNK), 1)
        want = r + k * (2 * CAP)
        for j in range(1, NZ):
            want += jnp.where(r >= j * 2 * CAP, ZSLOTS - 2 * CAP, 0)
        pick = jnp.where(m == want, 1.0, 0.0).astype(BF16)
        return jnp.dot(pick, zarr[p], preferred_element_type=F32).astype(BF16)

    def out_of_order(p):
        @pl.loop(0, NX)
        def _(k):
            m = lax.broadcasted_iota(jnp.int32, (CHUNK, NX * CHUNK), 0)
            r = lax.broadcasted_iota(jnp.int32, (CHUNK, NX * CHUNK), 1)
            upper = m >= ZSLOTS
            within = m - jnp.where(upper, ZSLOTS, 0)
            want = within + (2 * k + jnp.where(upper, 1, 0)) * (2 * CAP)
            for j in range(1, NX):
                want += jnp.where(within >= j * 2 * CAP, CHUNK - 2 * CAP, 0)
            pick = jnp.where(r == want, 1.0, 0.0).astype(BF16)
            rows = jnp.dot(pick, arr[p, :, MAIN:], preferred_element_type=F32)
            zarr[p, pl.ds(pl.multiple_of(k * CHUNK, CHUNK), CHUNK), :] = rows.astype(BF16)

    def zback(p, some):
        here = pl.ds(pl.multiple_of(z * ZSLOTS, ZSLOTS), ZSLOTS)
        for dz in some:
            there = pl.ds(pl.multiple_of(at_z(dz) * ZSLOTS, ZSLOTS), ZSLOTS)
            put(("zt", p), ("zt", p), zarr.at[p, there], zret.at[p, here], {"z": at_z(dz)})

    def zcombine(p):
        mine = pl.ds(pl.multiple_of(z * ZSLOTS, ZSLOTS), ZSLOTS)
        zret[p, mine, :] = zarr[p, mine, :]
        arrived(("zt", p), zsend.at[p])
        for xs in range(NX):
            share = jnp.concatenate(
                [
                    jnp.where(
                        zslot_iota == ztgt_v[p, pl.ds(xs * NZ + ze, 1), :], zwgt_v[p, pl.ds(xs * NZ + ze, 1), :], 0.0
                    )
                    for ze in range(NZ)
                ],
                axis=0,
            ).T.astype(BF16)
            got = jnp.dot(share, zret[p], preferred_element_type=F32)
            xg[p, xs * 128 : (xs + 1) * 128, :] = got.astype(BF16)
        for xs in range(NX):
            away = pl.ds(pl.multiple_of(xs * 128 + (1 - c) * ROWS, ROWS), ROWS)
            put(("xd", p), ("xd", p), xg.at[p, away], xd.at[p, pl.ds(xs * ROWS, ROWS)], {"core": 1 - c})
        arrived(("xd", p), xd.at[p])
        for xs in range(NX):
            land = pl.ds(xs * ROWS, ROWS)
            stay = pl.ds(pl.multiple_of(xs * 128 + c * ROWS, ROWS), ROWS)
            xg[p, stay, :] = (xg[p, stay, :].astype(F32) + xd[p, land, :].astype(F32)).astype(BF16)
        for d in (2, 1, 3):
            block = pl.ds(pl.multiple_of((at_x(d) * 2 + c) * ROWS, ROWS), ROWS)
            put(("xr", p), ("xr", p), xg.at[p, block], xr.at[p, d - 1], {"x": at_x(d)})

    def zowned(p):
        total = xg[p, pl.ds(pl.multiple_of((x * 2 + c) * ROWS, ROWS), ROWS), :].astype(F32)
        arrived(("xr", p), xr.at[p])
        for d in (1, 2, 3):
            total += xr[p, d - 1].astype(F32)
        return total

    pick = picker(0, 0)
    for q in range(1, len(FIRST)):
        arrived(("cot", FIRST[q][0]), gout_v.at[:, pl.ds(*FIRST[q])])
        start_ring(0, q, gout_v)
        if q == len(FIRST) - 2:
            step(0, 1, 0)
    for q in range(len(FIRST)):
        if q > 0:
            step(0, 1, q)
        settle(0, 1, q)
        dispatch(0, 0, q, pick)
    relay(0)

    arrived("delta", drecv_v)
    loads["ref"].wait()
    loads["gain"].wait()
    inputs = ref_v[...].astype(F32) + drecv_v[...].astype(F32) * jnp.where(s > 0, 1.0, 0.0)
    inputs_v[...] = inputs
    inverse = lax.rsqrt(jnp.mean(inputs * inputs, axis=-1, keepdims=True) + EPSILON)
    norm_v[...] = (inputs * inverse * gain_v[...]).astype(BF16)

    for p, (routes, probs) in enumerate(in_lanes(across_v, NX)):
        expert = (lax.broadcasted_iota(jnp.int32, (NZ, 8, 128), 0) * 2 + x * 16 + c).astype(F32)
        hits = [routes[xs][None] == expert for xs in range(NX)]
        tables(p, hits, [probs[xs][None] for xs in range(NX)], zshift, ztgt_v, zwgt_v)

    for n in (1, 2, 3):
        for q in range(len(FIRST)):
            step(0, n + 1, q)
        if n == 2:
            for q in range(len(HALVES)):
                start_ring(1, q, norm_v)
            spread(1, norm_v)
        for q in range(len(FIRST)):
            settle(0, n + 1, q)
        dispatch(0, n, 0, picker(0, n))
    zslots(0)
    for n in range(4):
        for q in range(len(HALVES)):
            step(1, n + 1, q)
        zpush(0, ((1, 7), (2, 6), (3, 5), (4,))[n])
        for q in range(len(HALVES)):
            settle(1, n + 1, q)
        dispatch(1, n, 0, picker(1, n))
        if n == 0:
            relay(1)
        if n == 2:
            zslots(1)
    zpush(1, (4, 3, 5, 2, 6, 1, 7))

    def slots_arrived(p):
        arrived(("x", p), send.at[p])
        arrived(("zs", p), zsend.at[p])

    across = (((1,), (1,)), ((), ()))

    slots_arrived(0)
    for k in names[9:]:
        loads[k].wait()

    @pl.loop(0, NX // 2)
    def _(k):
        at = pl.ds(pl.multiple_of(k * (2 * CHUNK), 2 * CHUNK), 2 * CHUNK)
        for j in (0, 1):
            part = pl.ds(pl.multiple_of((2 * k + j) * CHUNK, CHUNK), CHUNK)
            arr[0, part, MAIN:] = in_order(0, 2 * k + j)
        hidden = lax.dot_general(arr[0, at, :], down_v[...], across, preferred_element_type=F32)
        gate_act = pre_v[at, :ffn].astype(F32)
        up_act = pre_v[at, ffn:].astype(F32)
        sigma = jax.nn.sigmoid(gate_act)
        grad_gate = (hidden * up_act * sigma * (1.0 + gate_act * (1.0 - sigma))).astype(BF16)
        grad_up = (hidden * gate_act * sigma).astype(BF16)
        for j in range(0, width, COLS):
            total = lax.dot_general(grad_gate, gate_v[j : j + COLS, :], across, preferred_element_type=F32)
            total += lax.dot_general(grad_up, up_v[j : j + COLS, :], across, preferred_element_type=F32)
            arr[0, at, j : j + COLS] = total.astype(BF16)

    def back_chunks(p, n):
        return LAST if (p, n) == (1, 3) else WHOLE

    def give_back(p, some):
        for n in some:
            g = order[3 - n]
            for q, cols in enumerate(back_chunks(p, n)):
                cols = pl.ds(*cols)
                for d in (1, 2, 3):
                    where = pl.ds(pl.multiple_of(at_x(d) * CHUNK + g * SLOTS, 16), SLOTS)
                    land = pl.ds(pl.multiple_of(n * CHUNK + x * SLOTS, 16), SLOTS)
                    put(("t", p), ("t", p, n, q), arr.at[p, where, cols], ret.at[p, land, cols], {"x": at_x(d)})

    give_back(0, (0, 1, 2, 3))
    out_of_order(0)
    zback(0, (4, 3, 5, 2, 6, 1, 7))

    slots_arrived(1)

    @pl.loop(0, NX)
    def _(k):
        at = pl.ds(pl.multiple_of(k * CHUNK, CHUNK), CHUNK)
        arr[1, at, MAIN:] = in_order(1, k)
        rows = arr[1, at, :]
        gate_act = jnp.dot(rows, gate_v[...], preferred_element_type=F32)
        up_act = jnp.dot(rows, up_v[...], preferred_element_type=F32)
        hidden = (gate_act * jax.nn.sigmoid(gate_act) * up_act).astype(BF16)
        for j in range(0, width, COLS):
            total = jnp.dot(hidden, down_v[:, j : j + COLS], preferred_element_type=F32)
            arr[1, at, j : j + COLS] = total.astype(BF16)

    give_back(1, (0, 1, 2))
    out_of_order(1)

    for p in (0, 1):
        sent(("ring", p), ag.at[p, pl.ds(0, 15 * ROWS)])
        sent(("xg", p), xg.at[p, pl.ds(0, 7 * ROWS)])

    def shares(p, n):
        g = order[3 - n]
        return jnp.concatenate(
            [
                jnp.where(slot_iota == row_pair(tgt_v, p, xe, g), row_pair(wgt_v, p, xe, g), 0.0)
                for xe in range(NX)
            ],
            axis=0,
        ).T.astype(BF16)

    def weigh(p, n, q, share):
        g = order[3 - n]
        start, size = back_chunks(p, n)[q]
        part = pl.ds(start, size)
        arrived(("t", p, n, q), ret.at[p, pl.ds(n * CHUNK, 3 * SLOTS), part])
        mine = pl.ds(pl.multiple_of(n * CHUNK + x * SLOTS, 16), SLOTS)
        here = pl.ds(pl.multiple_of(x * CHUNK + g * SLOTS, 16), SLOTS)
        ret[p, mine, part] = arr[p, here, part]
        tokens = pl.ds(pl.multiple_of(g * TOKENS, TOKENS), TOKENS)
        for k in range(start, start + size, COLS):
            cols = pl.ds(k, min(COLS, start + size - k))
            got = jnp.dot(share, ret[p, pl.ds(n * CHUNK, CHUNK), cols], preferred_element_type=F32)
            ag[p, tokens, cols] = got.astype(BF16)
        for h in (0, 1):
            away = pl.ds(pl.multiple_of(g * TOKENS + h * 128 + (1 - c) * ROWS, ROWS), ROWS)
            put(
                ("d", p), ("d", p, n, q), ag.at[p, away, part], d2.at[p, pl.ds((n * 2 + h) * ROWS, ROWS), part],
                {"core": 1 - c},
            )

    def add_core(p, n, q):
        g = order[3 - n]
        part = pl.ds(*back_chunks(p, n)[q])
        arrived(("d", p, n, q), d2.at[p, pl.ds(n * 2 * ROWS, 2 * ROWS), part])
        for h in (0, 1):
            land = pl.ds((n * 2 + h) * ROWS, ROWS)
            stay = pl.ds(pl.multiple_of(g * TOKENS + h * 128 + c * ROWS, ROWS), ROWS)
            ag[p, stay, part] = (ag[p, stay, part].astype(F32) + d2[p, land, part].astype(F32)).astype(BF16)

    def combine(p, n, q, share):
        weigh(p, n, q, share)
        add_core(p, n, q)

    def place(k):
        return k - 1 if k > 0 else 3 - k

    def pass_chunks(p, k):
        return back_chunks(p, 3) if k in (3, 4, -2, -3) else WHOLE

    def pass_on(p, k, q=0):
        there = rows_of(at_z(5 - k) if k > 0 else at_z(-4 - k), c)
        part = pl.ds(*pass_chunks(p, k)[q])
        if k not in (1, -1):
            last = k - 1 if k > 0 else k + 1
            split = pass_chunks(p, last)
            if q < len(split):
                arrived(("r", p, last, q), rs.at[p, place(last), :, pl.ds(*split[q])])
            ag[p, there, part] = (ag[p, there, part].astype(F32) + rs[p, place(last), :, part].astype(F32)).astype(BF16)
        put(("r", p), ("r", p, k, q), ag.at[p, there, part], rs.at[p, place(k), :, part], {"z": at_z(1 if k > 0 else -1)})

    def owned(p, q):
        part = pl.ds(*back_chunks(p, 3)[q])
        for k in (4, -3):
            arrived(("r", p, k, q), rs.at[p, place(k), :, part])
        total = ag[p, rows_of(z, c), part].astype(F32)
        return total + rs[p, place(4), :, part].astype(F32) + rs[p, place(-3), :, part].astype(F32)

    def pass_pair(p, k):
        for q in range(len(pass_chunks(p, k))):
            pass_on(p, 1 - k, q)
            pass_on(p, k, q)

    zback(1, (1, 7, 2, 6))
    combine(0, 0, 0, shares(0, 0))
    pass_on(0, 1)
    zback(1, (3, 5))
    combine(0, 1, 0, shares(0, 1))
    pass_on(0, -1)
    zback(1, (4,))
    zcombine(0)
    give_back(1, (3,))
    combine(0, 2, 0, shares(0, 2))
    pass_on(0, 2)
    combine(0, 3, 0, shares(0, 3))
    pass_pair(0, 3)
    zcombine(1)
    combine(1, 0, 0, shares(1, 0))
    pass_on(1, 1)
    pass_pair(0, 4)
    combine(1, 1, 0, shares(1, 1))
    pass_on(1, -1)
    pass_on(1, 2)
    combine(1, 2, 0, shares(1, 2))
    for q in range(len(LAST)):
        pass_on(1, -2, q)

    acc_v[:, :MAIN] = owned(0, 0)
    acc_v[:, MAIN:] = zowned(0)
    weighted = acc_v[...] * gain_v[...]
    saved = saved_v[...].astype(F32)
    scale = lax.rsqrt(jnp.mean(saved * saved, axis=-1, keepdims=True) + EPSILON)
    projection = jnp.mean(weighted * saved, axis=-1, keepdims=True)
    out_o[1] = (
        gout_v[...].astype(F32) + scale * weighted - saved * (scale * scale * scale * projection)
    ).astype(BF16)

    for q in range(len(LAST)):
        pass_on(1, 3, q)
    share = shares(1, 3)
    weigh(1, 3, 0, share)
    for q in range(len(LAST)):
        if q + 1 < len(LAST):
            weigh(1, 3, q + 1, share)
        add_core(1, 3, q)
        pass_on(1, -3, q)
        pass_on(1, 4, q)
    for q, cols in enumerate(LAST):
        cols = pl.ds(*cols)
        out_o[0, :, cols] = (inputs_v[:, cols] + owned(1, q)).astype(BF16)
    out_o[0, :, MAIN:] = (inputs_v[:, MAIN:] + zowned(1)).astype(BF16)

    sent("cot", gout_v)
    sent("delta", dsend_v)
    sent("meta", meta_v.at[pl.ds(0, 15)])
    sent("across", across_v.at[pl.ds(0, 7)])
    for p in (0, 1):
        for kind, like in (
            ("x", send), ("t", send), ("zs", zsend), ("zt", zsend), ("d", d2), ("r", rs), ("xd", xd), ("xr", xr),
        ):
            sent((kind, p), like.at[p])
    assert (len(sents), len(arrivals)) == (N_SENT, N_ARRIVED), (len(sents), len(arrivals))


def on_device(
    reference_act, codes, scale_index, scale_table, norm_gain, routes_fwd, probs_fwd,
    gate_weight, up_weight, down_weight, saved_input, routes_bwd, probs_bwd, saved_preact, cotangent,
):
    width, ffn = gate_weight.shape[2:]
    slots = NX * CHUNK
    dma = pltpu.SemaphoreType.DMA
    both = pl.pallas_call(
        kernel,
        name="relay_moe",
        out_shape=jax.ShapeDtypeStruct((2, ROWS, width), BF16),
        in_specs=[pl.BlockSpec(memory_space=pl.ANY)] * 15,
        out_specs=pl.BlockSpec(memory_space=pltpu.VMEM),
        scratch_shapes=[
            pltpu.VMEM((ROWS, width), BF16),
            pltpu.VMEM((ROWS, width), jnp.int32),
            pltpu.VMEM((1, ROWS), jnp.int32),
            pltpu.VMEM((1, 16), F32),
            pltpu.VMEM((1, width), F32),
            pltpu.VMEM((8, ROWS), jnp.int32),
            pltpu.VMEM((8, ROWS), jnp.int32),
            pltpu.VMEM((8, ROWS), F32),
            pltpu.VMEM((8, ROWS), F32),
            pltpu.VMEM((ROWS, width), BF16),
            pltpu.VMEM((width, ffn), BF16),
            pltpu.VMEM((width, ffn), BF16),
            pltpu.VMEM((ffn, width), BF16),
            pltpu.VMEM((slots, 2 * ffn), BF16),
            pltpu.VMEM((ROWS, width), BF16),
            pltpu.VMEM((ROWS, width), BF16),
            pltpu.VMEM((ROWS, width), BF16),
            pltpu.VMEM((ROWS, width), BF16),
            pltpu.VMEM((ROWS, width), F32),
            pltpu.VMEM((16, 16, 128), F32),
            pltpu.VMEM((2, NX * NZ, 128), F32),
            pltpu.VMEM((2, NX * NZ, 128), F32),
            pltpu.VMEM((8, 16, 128), F32),
            pltpu.VMEM((2, NX * NZ, 128), F32),
            pltpu.VMEM((2, NX * NZ, 128), F32),
            pltpu.VMEM((ROWS, width), F32),
            pltpu.VMEM((2, 16 * ROWS, MAIN), BF16),
            pltpu.VMEM((2, 12 * SLOTS, MAIN), BF16),
            pltpu.VMEM((2, slots, width), BF16),
            pltpu.VMEM((2, slots, MAIN), BF16),
            pltpu.VMEM((2, NZ * ROWS, MAIN), BF16),
            pltpu.VMEM((2, 7, ROWS, MAIN), BF16),
            pltpu.VMEM((2, 8 * ROWS, SIDE), BF16),
            pltpu.VMEM((2, 7 * ZSLOTS, SIDE), BF16),
            pltpu.VMEM((2, NZ * ZSLOTS, SIDE), BF16),
            pltpu.VMEM((2, NZ * ZSLOTS, SIDE), BF16),
            pltpu.VMEM((2, NX * ROWS, SIDE), BF16),
            pltpu.VMEM((2, 3, ROWS, SIDE), BF16),
            dma((14,)), dma((N_SENT,)), dma((N_ARRIVED,)),
        ],
        compiler_params=pltpu.CompilerParams(
            collective_id=0, has_side_effects=True, vmem_limit_bytes=67_043_328
        ),
    )(
        reference_act[0], codes[0], scale_index, scale_table[None], norm_gain,
        routes_bwd[0].T, routes_fwd[0].T, probs_bwd[0].T, probs_fwd[0].T, saved_input[0], cotangent[0],
        gate_weight[0, 0], up_weight[0, 0], down_weight[0, 0], saved_preact[0, 0],
    )
    return both[0:1], both[1:2]


def solution(mesh):
    grid = jax.sharding.Mesh(
        mesh.devices.reshape(4, NX, NZ, 2), ("section", "x", "z", "core")
    )
    tokens = ("x", "z", "core")
    return jax.shard_map(
        on_device,
        mesh=grid,
        in_specs=(
            P("section", tokens, None),
            P("section", tokens, None),
            P("section", tokens),
            P(),
            P("section", None),
            P("section", tokens, None),
            P("section", tokens, None),
            P("section", tokens, None, None),
            P("section", tokens, None, None),
            P("section", tokens, None, None),
            P("section", tokens, None),
            P("section", tokens, None),
            P("section", tokens, None),
            P("section", tokens, None, None),
            P("section", tokens, None),
        ),
        out_specs=(P("section", tokens, None), P("section", tokens, None)),
        check_vma=False,
    )
```
